256 devices in a mesh: ctx: 32 (over z, x), ch: 8 (over y, core).
Axes of the slice: x: 4, y: 4, z: 8, core: 2. Of those that a mesh axis runs over, the one named last changes fastest.
Arguments:
- featurized: bfloat16 [3, 1024, 16384], P(None, 'ch', 'ctx'), may hold values from -6 to 6
- short_weights: float32 [3, 1024, 3], P(None, 'ch'), may hold values from -3.5 to 3.5
- filter_taps: float32 [1024, 16384], P('ch', 'ctx'), may hold values from -5 to 5
- skip_gain: float32 [1024], P('ch'), may hold values from 0.5 to 1.5
- w_out: bfloat16 [1024, 1024], P('ch'), may hold values from -0.1875 to 0.1875
Outputs:
- mixed: bfloat16 [1024, 16384], P('ch', 'ctx')
The draws below stay inside these ranges and needn't reach their ends.
All inputs are finite; a program needn't handle non-finite values.
Results may differ from the reference program's by a relative error of at most 0.0089.
Values may be sent and summed in bfloat16 or wider, within the bound.
A program may use at most 64 MiB of HBM per device.

```python
import jax
import jax.numpy as jnp
from jax import lax

FEATURE_WIDTH = 1024
KSHORT = 3
TOKEN_SPAN = 16384
FFTLEN = 32768


def unit_rows(envelope):
    return envelope * jax.lax.rsqrt(jnp.sum(envelope * envelope, axis=1, keepdims=True))


def draw_filter_taps(key, part):
    stochastic_seeds = jax.random.split(jax.random.fold_in(key, 17), 5)
    slow_share = 0.5
    is_slow = jax.random.uniform(stochastic_seeds[0], (FEATURE_WIDTH,)) < slow_share
    slow_low = jnp.log(TOKEN_SPAN / 2.0)
    slow_high = jnp.log(TOKEN_SPAN * 8.0)
    slow_reach = jnp.exp(slow_low + (slow_high - slow_low) * jax.random.uniform(stochastic_seeds[1], (FEATURE_WIDTH,)))
    fast_low = jnp.log(30.0)
    fast_high = jnp.log(50.0)
    fast_reach = jnp.exp(fast_low + (fast_high - fast_low) * jax.random.uniform(stochastic_seeds[4], (FEATURE_WIDTH,)))
    retard_shifts = jnp.arange(TOKEN_SPAN, dtype=jnp.float32)
    slow_shape = unit_rows(jnp.exp(-retard_shifts[None, :] / slow_reach[:, None]))
    fast_shape = unit_rows(jnp.exp(-retard_shifts[None, :] / fast_reach[:, None]))
    blended = jnp.sqrt(0.6) * fast_shape + jnp.sqrt(0.4) * slow_shape
    envelope = jnp.where(is_slow[:, None], slow_shape, blended)
    cluster_bundles = jax.random.randint(stochastic_seeds[2], (FEATURE_WIDTH, 3), 0, TOKEN_SPAN).astype(jnp.float32)
    bypass_carried = jnp.zeros((FEATURE_WIDTH, TOKEN_SPAN), jnp.float32)
    for bucket_ordinal in range(3):
        bypass_carried = bypass_carried + (retard_shifts[None, :] >= cluster_bundles[:, bucket_ordinal:bucket_ordinal + 1]).astype(jnp.float32)
    envelope = envelope * jnp.power(0.6, bypass_carried)
    random_part = jax.random.truncated_normal(stochastic_seeds[3], -4.0, 4.0, (FEATURE_WIDTH, TOKEN_SPAN), jnp.float32)
    return (random_part * unit_rows(envelope)).astype(jnp.float32)


def block_scale(own_key, extent, cuts, least, top_value):
    factor_of, own = 1.0, jax.random.fold_in(own_key, 6)
    for position, shards_of in cuts:
        heights = jnp.exp(jax.random.uniform(jax.random.fold_in(own, position), (shards_of,), jnp.float32, least / len(cuts), top_value / len(cuts)))
        factor_of = factor_of * jnp.repeat(heights, extent[position] // shards_of).reshape([-1 if axis == position else 1 for axis in range(len(extent))])
    return factor_of


def gaussian(rng, extent, deviation, limit, pieces=(), kind=jnp.bfloat16):
    entries = jax.random.normal(rng, extent, jnp.float32) * deviation
    if len(pieces) > 0:
        entries = block_scale(rng, extent, pieces, -0.22, 0.18) * entries
    return jnp.clip(entries, min=-limit, max=limit).astype(kind)


def setup_inputs(seed: int = 0) -> dict:
    arg_keys = jax.random.split(jax.random.key(seed), 6)
    return {
        "featurized": gaussian(arg_keys[0], (3, FEATURE_WIDTH, TOKEN_SPAN), 1.0, 6.0, ((1, 8), (2, 32))),
        "short_weights": gaussian(arg_keys[1], (3, FEATURE_WIDTH, KSHORT), KSHORT ** -0.5, 3.5, ((1, 8),), jnp.float32),
        "filter_taps": draw_filter_taps(jax.random.fold_in(arg_keys[5], 71), 0),
        "skip_gain": jnp.clip(0.5 + 1.0 * jax.random.uniform(arg_keys[3], (FEATURE_WIDTH,), jnp.float32) ** block_scale(arg_keys[3], (FEATURE_WIDTH,), ((0, 8),), -0.2, 0.2), 0.5, 1.5),
        "w_out": gaussian(arg_keys[4], (FEATURE_WIDTH, FEATURE_WIDTH), FEATURE_WIDTH ** -0.5, 0.1875, ((0, 8),)),
    }


def causal_short(featurized, short_weights):
    width = short_weights.shape[2]
    values = featurized.astype(jnp.float32)
    length = values.shape[2]
    padded = jnp.pad(values, ((0, 0), (0, 0), (width - 1, 0)))
    filtered = jnp.zeros(values.shape, jnp.float32)
    for offset in range(width):
        begin = width - 1 - offset
        filtered = filtered + short_weights[:, :, offset:offset + 1] * padded[:, :, begin:begin + length]
    return filtered


def long_block(operands):
    gated, taps = operands
    length = gated.shape[1]
    spectrum = jnp.fft.rfft(gated, n=FFTLEN, axis=1) * jnp.fft.rfft(taps, n=FFTLEN, axis=1)
    return jnp.fft.irfft(spectrum, n=FFTLEN, axis=1)[:, :length].astype(jnp.float32)


def reference(featurized, short_weights, filter_taps, skip_gain, w_out):
    filtered = causal_short(featurized, short_weights)
    gated = filtered[1] * filtered[2]
    group = 128 if FEATURE_WIDTH % 128 == 0 else FEATURE_WIDTH
    blocks = FEATURE_WIDTH // group
    conv = lax.map(long_block, (gated.reshape(blocks, group, TOKEN_SPAN), filter_taps.reshape(blocks, group, TOKEN_SPAN)))
    conv = conv.reshape(FEATURE_WIDTH, TOKEN_SPAN)
    hidden_mix = (filtered[0] * (conv + skip_gain[:, None] * gated)).astype(jnp.bfloat16)
    return jnp.dot(w_out, hidden_mix, preferred_element_type=jnp.float32).astype(jnp.bfloat16)
```

```python
import math

import jax
import jax.numpy as jnp
import numpy as np
from jax import lax
from jax.experimental import pallas as pl
from jax.experimental.pallas import tpu as pltpu
from jax.sharding import PartitionSpec as P

NP = 32
NC = 4
MESH = pl.DeviceIdType.MESH
F32 = jnp.float32
BF16 = jnp.bfloat16


def split(table):
    high = table.astype(BF16)
    return high, (table - high.astype(np.float32)).astype(BF16)


def tables():
    index = np.arange(128)
    first = 4 * (index % NP) + index // NP
    one = 2 * math.pi * (((4 * index[:, None] + 1) * first[None, :]) % 512) / 512
    two = 2 * math.pi * ((index[:, None] * index[None, :]) % 128) / 128
    twist = 2 * math.pi * (((4 * index[:, None] + 1) * index[None, :]) % 65536) / 65536
    c2, s2 = np.cos(two), np.sin(two)
    f32 = np.float32
    e1 = np.concatenate([np.cos(one), -np.sin(one)], 0).astype(f32)
    m2 = np.block([[c2, -s2], [s2, c2]]).astype(f32)
    m3 = np.block([[c2, s2], [-s2, c2]]).astype(f32)
    back = (np.concatenate([np.cos(one).T, -np.sin(one).T], 1) / 16384).astype(f32)
    e1_high, e1_low = split(e1)
    return (
        np.concatenate([e1_high, e1_low], 1),
        np.stack(split(m2)),
        np.stack(split(m3)),
        np.stack(split(back)),
        np.stack([np.cos(twist), -np.sin(twist)]).astype(f32),
    )


def dot(left, right):
    return jnp.dot(left, right, preferred_element_type=F32)


def halves(value):
    high = value.astype(BF16)
    return high, (value - high.astype(F32)).astype(BF16)


def forward(rows, e1, m2, twist):
    parts = []
    for c in range(NC):
        parts.append(
            jnp.concatenate([rows[pl.ds(4 * c + a, NP, stride=16), :] for a in range(4)], 0)
        )
    grid = jnp.concatenate(parts, 1).astype(BF16)
    mixed = dot(e1[...], jnp.concatenate([grid, grid], 0))
    tr, ti = twist[0], twist[1]
    turned = []
    for c in range(NC):
        re, im = mixed[:128, 128 * c : 128 * c + 128], mixed[128:, 128 * c : 128 * c + 128]
        turned.append(jnp.concatenate([re * tr - im * ti, re * ti + im * tr], 1))
    high, low = halves(jnp.concatenate(turned, 0))
    return dot(high, m2[0]) + dot(low, m2[0]) + dot(high, m2[1])


def inverse(spectrum, rows, m3, back, twist):
    high, low = halves(spectrum)
    mixed = dot(high, m3[0]) + dot(low, m3[0]) + dot(high, m3[1])
    tr, ti = twist[0], twist[1]
    turned = []
    for c in range(NC):
        re, im = mixed[128 * c : 128 * c + 128, :128], mixed[128 * c : 128 * c + 128, 128:]
        turned.append(jnp.concatenate([re * tr + im * ti, im * tr - re * ti], 0))
    high, low = halves(jnp.concatenate(turned, 1))
    done = dot(back[0], high) + dot(back[1], high) + dot(back[0], low)
    for c in range(NC):
        for a in range(4):
            rows[pl.ds(4 * c + a, NP, stride=16), :] = done[
                NP * a : NP * a + NP, 128 * c : 128 * c + 128
            ]


def product(g, h):
    gr, gi, hr, hi = g[:, :128], g[:, 128:], h[:, :128], h[:, 128:]
    return jnp.concatenate([gr * hr - gi * hi, gr * hi + gi * hr], 1)


def kernel(
    feat, taps, sw, skip, w, e1h, m2h, m3h, bkh, twh, out,
    fv, tv, swv, skv, wv, e1, m2, m3, bk, tw,
    halo, cols, f0, gt, rows, hsend, hrecv, gsend, grecv, csend, crecv, spec, ag,
    lsem, osem, rsem, asem, arem,
):
    me = lax.axis_index("ctx")
    ch = lax.axis_index("ch")
    y, core = ch // 2, ch % 2
    partner = 2 * y + 1 - core
    up, down = (y + 1) % 4 * 2 + core, (y + 3) % 4 * 2 + core
    across = (y + 2) % 4 * 2 + core

    local = [
        pltpu.make_async_copy(s, d, lsem.at[i])
        for i, (s, d) in enumerate(
            [(taps, tv), (feat, fv), (sw, swv), (skip, skv), (e1h, e1), (m2h, m2), (twh, tw),
             (m3h, m3), (bkh, bk), (w, wv)]
        )
    ]
    for c in local:
        c.start()

    barrier = pltpu.get_barrier_semaphore()

    def greet(i, _):
        pl.semaphore_signal(
            barrier, inc=1, device_id={"ctx": (me + i) % NP}, device_id_type=MESH
        )
        return 0

    lax.fori_loop(1, NP, greet, 0)
    for other in (partner, up, down):
        pl.semaphore_signal(barrier, inc=1, device_id={"ch": other}, device_id_type=MESH)

    def lay(ref, send):
        send[...] = ref[...].astype(BF16).reshape(NP, 16, 128)

    local[0].wait()
    for a in range(4):
        rows[pl.ds(a, 128, stride=4), :] = tv[:, 128 * a : 128 * a + 128]
    lay(rows, hsend)
    hrecv[me] = hsend[me]
    local[1].wait()
    pl.semaphore_wait(barrier, NP - 1 + 3)

    rim = pltpu.make_async_remote_copy(
        fv.at[:, :, pl.ds(384, 128)], halo, osem.at[3], rsem.at[3],
        device_id={"ctx": (me + 1) % NP}, device_id_type=MESH,
    )
    rim.start()

    def spread(send, recv, k):
        def one(i, _):
            peer = (me + i) % NP
            pltpu.make_async_remote_copy(
                send.at[peer], recv.at[me], osem.at[k], rsem.at[k],
                device_id={"ctx": peer}, device_id_type=MESH,
            ).start()
            return 0

        lax.fori_loop(1, NP, one, 0)

    def arrived(buf, sem):
        part = buf.at[pl.ds(0, NP - 1)]
        pltpu.make_async_copy(part, part, sem).wait()

    spread(hsend, hrecv, 0)

    local[2].wait()
    local[3].wait()
    cols[...] = jnp.zeros_like(cols)
    for s in range(3):
        for j in range(3):
            cols[pl.ds(3 * s + j, 1), :] = swv[s, pl.ds(j, 1), :]
    cols[pl.ds(9, 1), :] = skv[...]
    col = cols[...].T
    rim.wait()
    inside = me > 0

    def short(s):
        edge = jnp.where(inside, halo[s].astype(F32), 0.0)
        wide = jnp.concatenate([edge, fv[s].astype(F32)], 1)
        total = col[:, 3 * s : 3 * s + 1] * wide[:, 128:]
        for j in (1, 2):
            moved = pltpu.roll(wide, j, 1)[:, 128:]
            total = total + col[:, 3 * s + j : 3 * s + j + 1] * moved
        return total

    gt[...] = short(1) * short(2)
    for a in range(4):
        rows[pl.ds(a, 128, stride=4), :] = gt[:, 128 * a : 128 * a + 128]
    lay(rows, gsend)
    grecv[me] = gsend[me]
    spread(gsend, grecv, 1)
    f0[...] = short(0)
    gt[...] = col[:, 9:10] * gt[...]

    for c in local[4:]:
        c.wait()
    arrived(hrecv, rsem.at[0])
    rows[...] = hrecv[...].reshape(512, 128).astype(F32)
    spec[...] = forward(rows, e1, m2, tw)
    arrived(grecv, rsem.at[1])
    rows[...] = grecv[...].reshape(512, 128).astype(F32)
    inverse(product(forward(rows, e1, m2, tw), spec[...]), rows, m3, bk, tw)
    lay(rows, csend)
    crecv[me] = csend[me]
    spread(csend, crecv, 2)
    arrived(crecv, rsem.at[2])

    rows[...] = crecv[...].reshape(512, 128).astype(F32)
    for a in range(4):
        lanes = pl.ds(128 * a, 128)
        conv = rows[pl.ds(a, 128, stride=4), :]
        ag[ch, :, lanes] = (f0[:, lanes] * (conv + gt[:, lanes])).astype(BF16)

    def hand(block, half, k, other):
        piece = ag.at[block, pl.ds(64 * half, 64)]
        return pltpu.make_async_remote_copy(
            piece, piece, asem.at[k], arem.at[k], device_id={"ch": other}, device_id_type=MESH
        )

    sent = []

    def go(*args):
        copy = hand(*args)
        copy.start()
        sent.append(copy)

    def take(block, half, k):
        hand(block, half, k, partner).wait_recv()

    go(ch, 0, 0, up)
    go(ch, 1, 1, down)
    go(ch, 1, 2, up)
    go(ch, 0, 3, down)
    go(ch, 0, 4, partner)
    go(ch, 1, 5, partner)
    take(down, 0, 0)
    go(down, 0, 6, up)
    take(up, 1, 1)
    go(up, 1, 7, down)
    go(down, 0, 8, partner)
    go(up, 1, 9, partner)
    take(down, 1, 2)
    go(down, 1, 10, partner)
    take(up, 0, 3)
    go(up, 0, 11, partner)
    take(partner, 0, 4)
    take(partner, 1, 5)

    def pair(chip):
        both = ag[pl.ds(2 * chip, 2)].reshape(256, 512)
        return dot(wv[:, pl.ds(pl.multiple_of(256 * chip, 256), 256)], both)

    total = pair(y)
    twin_up, twin_down, twin_across = ((x // 2) * 2 + 1 - core for x in (up, down, across))
    take(across, 0, 6)
    go(across, 0, 12, partner)
    take(across, 1, 7)
    go(across, 1, 13, partner)
    take(twin_down, 0, 8)
    take(twin_up, 1, 9)
    take(twin_down, 1, 10)
    take(twin_up, 0, 11)
    total = total + pair(up // 2) + pair(down // 2)
    take(twin_across, 0, 12)
    take(twin_across, 1, 13)
    out[...] = (total + pair(across // 2)).astype(BF16)

    for copy in sent:
        copy.wait_send()
    arrived(hsend, osem.at[0])
    arrived(gsend, osem.at[1])
    arrived(csend, osem.at[2])


def local(featurized, short_weights, filter_taps, skip_gain, w_out):
    e1, m2, m3, back, twist = tables()
    any_space = pl.BlockSpec(memory_space=pl.ANY)
    V = pltpu.VMEM
    chunk = V((NP, 16, 128), BF16)
    return pl.pallas_call(
        kernel,
        out_shape=jax.ShapeDtypeStruct((128, 512), BF16),
        in_specs=[any_space] * 10,
        out_specs=pl.BlockSpec(memory_space=pltpu.VMEM),
        scratch_shapes=[
            V((3, 128, 512), BF16), V((128, 512), F32), V((3, 3, 128), F32), V((1, 128), F32),
            V((128, 1024), BF16), V(e1.shape, BF16), V(m2.shape, BF16), V(m3.shape, BF16),
            V(back.shape, BF16), V(twist.shape, F32),
            V((3, 128, 128), BF16), V((128, 128), F32), V((128, 512), F32), V((128, 512), F32),
            V((512, 128), F32), chunk, chunk, chunk, chunk, chunk, chunk,
            V((512, 256), F32), V((8, 128, 512), BF16),
            pltpu.SemaphoreType.DMA((10,)),
            pltpu.SemaphoreType.DMA((4,)),
            pltpu.SemaphoreType.DMA((4,)),
            pltpu.SemaphoreType.DMA((14,)),
            pltpu.SemaphoreType.DMA((14,)),
        ],
        compiler_params=pltpu.CompilerParams(collective_id=0, has_side_effects=True),
        name="hyena",
    )(
        featurized, filter_taps, jnp.swapaxes(short_weights, 1, 2), skip_gain.reshape(1, 128),
        w_out, e1, m2, m3, back, twist,
    )


def solution(mesh):
    in_specs = (P(None, "ch", "ctx"), P(None, "ch", None), P("ch", "ctx"), P("ch"), P("ch", None))
    out_specs = P("ch", "ctx")
    return jax.shard_map(local, mesh=mesh, in_specs=in_specs, out_specs=out_specs, check_vma=False)
```

```python
import math

import jax
import jax.numpy as jnp
import numpy as np
from jax import lax
from jax.experimental import pallas as pl
from jax.experimental.pallas import tpu as pltpu
from jax.sharding import PartitionSpec as P

NP = 32
NC = 4
FAR_H, FAR_G, FAR_C = False, True, False
MESH = pl.DeviceIdType.MESH
F32 = jnp.float32
BF16 = jnp.bfloat16


def split(table):
    high = table.astype(BF16)
    return high, (table - high.astype(np.float32)).astype(BF16)


def tables():
    index = np.arange(128)
    first = 4 * (index % NP) + index // NP
    one = 2 * math.pi * (((4 * index[:, None] + 1) * first[None, :]) % 512) / 512
    two = 2 * math.pi * ((index[:, None] * index[None, :]) % 128) / 128
    twist = 2 * math.pi * (((4 * index[:, None] + 1) * index[None, :]) % 65536) / 65536
    c2, s2 = np.cos(two), np.sin(two)
    f32 = np.float32
    e1 = np.concatenate([np.cos(one), -np.sin(one)], 0).astype(f32)
    m2 = np.block([[c2, -s2], [s2, c2]]).astype(f32)
    m3 = np.block([[c2, s2], [-s2, c2]]).astype(f32)
    back = (np.concatenate([np.cos(one).T, -np.sin(one).T], 1) / 16384).astype(f32)
    e1_high, e1_low = split(e1)
    return (
        np.concatenate([e1_high, e1_low], 1),
        np.stack(split(m2)),
        np.stack(split(m3)),
        np.stack(split(back)),
        np.stack([np.cos(twist), -np.sin(twist)]).astype(f32),
    )


def dot(left, right):
    return jnp.dot(left, right, preferred_element_type=F32)


def halves(value):
    high = value.astype(BF16)
    return high, (value - high.astype(F32)).astype(BF16)


def forward(rows, e1, m2, twist):
    parts = []
    for c in range(NC):
        parts.append(
            jnp.concatenate([rows[pl.ds(4 * c + a, NP, stride=16), :] for a in range(4)], 0)
        )
    grid = jnp.concatenate(parts, 1).astype(BF16)
    mixed = dot(e1[...], jnp.concatenate([grid, grid], 0))
    tr, ti = twist[0], twist[1]
    turned = []
    for c in range(NC):
        re, im = mixed[:128, 128 * c : 128 * c + 128], mixed[128:, 128 * c : 128 * c + 128]
        turned.append(jnp.concatenate([re * tr - im * ti, re * ti + im * tr], 1))
    high, low = halves(jnp.concatenate(turned, 0))
    return dot(high, m2[0]) + dot(low, m2[0]) + dot(high, m2[1])


def inverse(spectrum, rows, m3, back, twist):
    high, low = halves(spectrum)
    mixed = dot(high, m3[0]) + dot(low, m3[0]) + dot(high, m3[1])
    tr, ti = twist[0], twist[1]
    turned = []
    for c in range(NC):
        re, im = mixed[128 * c : 128 * c + 128, :128], mixed[128 * c : 128 * c + 128, 128:]
        turned.append(jnp.concatenate([re * tr + im * ti, im * tr - re * ti], 0))
    high, low = halves(jnp.concatenate(turned, 1))
    done = dot(back[0], high) + dot(back[1], high) + dot(back[0], low)
    for c in range(NC):
        for a in range(4):
            rows[pl.ds(a // 2 * 8 + 2 * c + a % 2, NP, stride=16), :] = done[
                NP * a : NP * a + NP, 128 * c : 128 * c + 128
            ]


def product(g, h):
    gr, gi, hr, hi = g[:, :128], g[:, 128:], h[:, :128], h[:, 128:]
    return jnp.concatenate([gr * hr - gi * hi, gr * hi + gi * hr], 1)


def plane_order(k):
    return (k + 1) // 2 * (2 * (k % 2) - 1)


def kernel(
    feat, taps, sw, skip, w, e1h, m2h, m3h, bkh, twh, out,
    fv, tv, swv, skv, wv, wr, e1, m2, m3, bk, tw,
    rimsend, rimrecv, cols, f0, gt, f0r, gtr, rows,
    hsend, hrecv, gsend, grecv, csend, crecv, spec, ag, fin, finr,
    lsem, osem, rsem, csem, asem, arem, psem, prem,
):
    me = lax.axis_index("ctx")
    ch = lax.axis_index("ch")
    x, z = me % 4, me // 4
    y, core = ch // 2, ch % 2
    partner = 2 * y + 1 - core
    up, down, across = ((y + d) % 4 * 2 + core for d in (1, 3, 2))

    local = [
        pltpu.make_async_copy(s, d, lsem.at[i])
        for i, (s, d) in enumerate(
            [(taps, tv), (feat, fv), (sw, swv), (skip, skv), (w, wv), (e1h, e1), (m2h, m2), (twh, tw),
             (m3h, m3), (bkh, bk)]
        )
    ]
    for c in local:
        c.start()

    barrier = pltpu.get_barrier_semaphore()

    def greet(i, _):
        for own in (ch, partner):
            pl.semaphore_signal(
                barrier, inc=1, device_id={"ctx": (me + i) % NP, "ch": own}, device_id_type=MESH
            )
        return 0

    lax.fori_loop(1, NP, greet, 0)
    for other in (partner, up, down, across):
        pl.semaphore_signal(barrier, inc=1, device_id={"ch": other}, device_id_type=MESH)

    local[0].wait()
    for a in range(4):
        rows[pl.ds(a, 128, stride=4), :] = tv[:, 128 * a : 128 * a + 128]
    hsend[...] = rows[...].astype(BF16).reshape(NP, 16, 128)
    hrecv[me] = hsend[me]
    local[1].wait()
    for s in range(3):
        rimsend[pl.ds(8 * s, 8), :] = fv[s, :, 384:].astype(F32).T[120:, :]
    local[4].wait()

    pl.semaphore_wait(barrier, 2 * (NP - 1) + 4)
    rim = pltpu.make_async_remote_copy(
        rimsend, rimrecv, osem.at[3], rsem.at[3],
        device_id={"ctx": (me + 1) % NP}, device_id_type=MESH,
    )
    rim.start()

    def spot(i, far):
        i = NP - i if far else i
        return (z + 8 + plane_order(i // 4)) % 8 * 4 + (x + i) % 4

    def spread(send, recv, k, far):
        def one(i, _):
            peer = spot(i, far)
            pltpu.make_async_remote_copy(
                send.at[peer], recv.at[me], osem.at[k], rsem.at[k],
                device_id={"ctx": peer}, device_id_type=MESH,
            ).start()
            return 0

        lax.fori_loop(1, NP, one, 0)

    def arrived(part, sem):
        pltpu.make_async_copy(part, part, sem).wait()

    def mates(i, source, target):
        return pltpu.make_async_remote_copy(
            source, target, psem.at[i], prem.at[i], device_id={"ch": partner}, device_id_type=MESH
        )

    most = pl.ds(0, NP - 1)
    spread(hsend, hrecv, 0, FAR_H)
    swap = [mates(0, wv, wr)]
    swap[0].start()

    local[2].wait()
    local[3].wait()
    cols[...] = jnp.zeros_like(cols)
    for s in range(3):
        for j in range(3):
            cols[pl.ds(3 * s + j, 1), :] = swv[s, pl.ds(j, 1), :]
    cols[pl.ds(9, 1), :] = skv[...]
    col = cols[...].T

    def short(s, edge, width):
        wide = jnp.concatenate([edge, fv[s, :, :width].astype(F32)], 1)
        total = col[:, 3 * s : 3 * s + 1] * wide[:, 128:]
        for j in (1, 2):
            moved = pltpu.roll(wide, j, 1)[:, 128:]
            total = total + col[:, 3 * s + j : 3 * s + j + 1] * moved
        return total

    nothing = jnp.zeros((128, 128), F32)
    gated = short(1, nothing, 512) * short(2, nothing, 512)
    gt[0], gt[1] = gated[:, :256], gated[:, 256:]
    for a in range(1, 4):
        rows[pl.ds(a, 128, stride=4), :] = gated[:, 128 * a : 128 * a + 128]

    rim.wait()
    inside = me > 0

    def edge(s):
        last = jnp.concatenate([jnp.zeros((120, 128), F32), rimrecv[pl.ds(8 * s, 8), :]], 0)
        return jnp.where(inside, last.T, 0.0)

    gt[0, :, :128] = short(1, edge(1), 128) * short(2, edge(2), 128)
    rows[pl.ds(0, 128, stride=4), :] = gt[0, :, :128]
    gsend[...] = rows[...].astype(BF16).reshape(NP, 16, 128)
    grecv[me] = gsend[me]
    spread(gsend, grecv, 1, FAR_G)
    for half in range(2):
        gt[half] = col[:, 9:10] * gt[half]
    whole = short(0, edge(0), 512)
    f0[0], f0[1] = whole[:, :256], whole[:, 256:]
    swap += [mates(1, gt.at[1 - core], gtr), mates(2, f0.at[1 - core], f0r)]
    swap[1].start()
    swap[2].start()

    for c in local[5:]:
        c.wait()
    arrived(hrecv.at[most], rsem.at[0])
    rows[...] = hrecv[...].reshape(512, 128).astype(F32)
    spec[...] = forward(rows, e1, m2, tw)
    for c in swap:
        c.wait_recv()
    arrived(grecv.at[most], rsem.at[1])
    rows[...] = grecv[...].reshape(512, 128).astype(F32)
    inverse(product(forward(rows, e1, m2, tw), spec[...]), rows, m3, bk, tw)

    csend[...] = rows[...].astype(BF16).reshape(NP, 2, 8, 128)
    crecv[core, me] = csend[me, core]

    def half_of(peer, half, sem):
        pltpu.make_async_remote_copy(
            csend.at[peer, half], crecv.at[core, me], sem, csem.at[z],
            device_id={"ctx": peer, "ch": 2 * y + half}, device_id_type=MESH,
        ).start()

    half_of(me, 1 - core, osem.at[4])

    def one(i, _):
        for half in range(2):
            half_of(spot(i, FAR_C), half, osem.at[2])
        return 0

    lax.fori_loop(1, NP, one, 0)

    def plane(k):
        return (z + 8 + plane_order(k)) % 8

    def hand(chip, k, t, other):
        piece = ag.at[pl.ds(2 * chip, 2), pl.ds(pl.multiple_of(16 * plane(k), 16), 16)]
        return pltpu.make_async_remote_copy(
            piece, piece, asem.at[t, k], arem.at[t, k], device_id={"ch": other}, device_id_type=MESH
        )

    sent = []
    for k in (range(7, -1, -1) if FAR_C else range(8)):
        first = plane(k)
        arrived(crecv.at[0, pl.ds(0, 8 if k else 7)], csem.at[first])
        here = pl.ds(pl.multiple_of(16 * first, 16), 16)
        for which, (block, f, g) in enumerate(
            [(core, f0.at[core], gt.at[core]), (1 - core, f0r, gtr)]
        ):
            base = 64 * k + 32 * which
            came = crecv[block, pl.ds(4 * first, 4)].reshape(32, 128)
            rows[pl.ds(base, 32), :] = came.astype(F32)
            for a in range(2):
                lanes = pl.ds(128 * a, 128)
                conv = rows[pl.ds(base + a, 16, stride=2), :]
                ag[2 * y + block, here, lanes] = (
                    f[here, lanes] * (conv + g[here, lanes])
                ).astype(BF16)
        for t, other in ((2, across), (0, up), (1, down)):
            copy = hand(y, k, t, other)
            copy.start()
            sent.append(copy)

    def pair(chip):
        both = ag[pl.ds(2 * chip, 2)].reshape(256, 256)
        columns = pl.ds(pl.multiple_of(256 * chip, 256), 256)
        return dot(jnp.concatenate([wr[:, columns], wv[:, columns]], 0), both)

    total = pair(y)
    for t, other in ((0, down), (1, up), (2, across)):
        for k in range(8):
            hand(other // 2, k, t, other).wait_recv()
        total = total + pair(other // 2)
    fin[...] = total[:128].astype(BF16)
    last = mates(3, fin, finr)
    last.start()
    mine = total[128:].astype(BF16)
    out[:, pl.ds(pl.multiple_of(256 * core, 256), 256)] = mine
    last.wait_recv()
    out[:, pl.ds(pl.multiple_of(256 * (1 - core), 256), 256)] = finr[...]

    for copy in sent + swap + [last]:
        copy.wait_send()
    arrived(hsend.at[most], osem.at[0])
    arrived(gsend.at[most], osem.at[1])
    arrived(csend.at[most], osem.at[2])
    arrived(csend.at[0, 0], osem.at[4])


def local(featurized, short_weights, filter_taps, skip_gain, w_out):
    e1, m2, m3, back, twist = tables()
    far = pl.BlockSpec(memory_space=pl.ANY)
    V = pltpu.VMEM
    chunk = V((NP, 16, 128), BF16)
    two = V((2, 128, 256), F32)
    half = V((128, 256), F32)
    return pl.pallas_call(
        kernel,
        out_shape=jax.ShapeDtypeStruct((128, 512), BF16),
        in_specs=[far] * 10,
        out_specs=pl.BlockSpec(memory_space=pltpu.VMEM),
        scratch_shapes=[
            V((3, 128, 512), BF16), V((128, 512), F32), V((3, 3, 128), F32), V((1, 128), F32),
            V((128, 1024), BF16), V((128, 1024), BF16),
            V(e1.shape, BF16), V(m2.shape, BF16), V(m3.shape, BF16),
            V(back.shape, BF16), V(twist.shape, F32),
            V((24, 128), F32), V((24, 128), F32), V((128, 128), F32),
            two, two, half, half, V((512, 128), F32), chunk, chunk, chunk, chunk,
            V((NP, 2, 8, 128), BF16), V((2, NP, 8, 128), BF16),
            V((512, 256), F32), V((8, 128, 256), BF16), V((128, 256), BF16), V((128, 256), BF16),
            pltpu.SemaphoreType.DMA((10,)),
            pltpu.SemaphoreType.DMA((5,)),
            pltpu.SemaphoreType.DMA((4,)),
            pltpu.SemaphoreType.DMA((8,)),
            pltpu.SemaphoreType.DMA((3, 8)),
            pltpu.SemaphoreType.DMA((3, 8)),
            pltpu.SemaphoreType.DMA((4,)),
            pltpu.SemaphoreType.DMA((4,)),
        ],
        compiler_params=pltpu.CompilerParams(collective_id=0, has_side_effects=True),
        name="hyena",
    )(
        featurized, filter_taps, jnp.swapaxes(short_weights, 1, 2), skip_gain.reshape(1, 128),
        w_out, e1, m2, m3, back, twist,
    )


def solution(mesh):
    in_specs = (P(None, "ch", "ctx"), P(None, "ch", None), P("ch", "ctx"), P("ch"), P("ch", None))
    out_specs = P("ch", "ctx")
    return jax.shard_map(local, mesh=mesh, in_specs=in_specs, out_specs=out_specs, check_vma=False)
```

```python
import math

import jax
import jax.numpy as jnp
import numpy as np
from jax import lax
from jax.experimental import pallas as pl
from jax.experimental.pallas import tpu as pltpu
from jax.sharding import PartitionSpec as P

NP = 32
NC = 4
FAR_H, FAR_G, FAR_C = False, True, False
MESH = pl.DeviceIdType.MESH
F32 = jnp.float32
BF16 = jnp.bfloat16


def split(table):
    high = table.astype(BF16)
    return high, (table - high.astype(np.float32)).astype(BF16)


def tables():
    index = np.arange(128)
    first = 4 * (index % NP) + index // NP
    one = 2 * math.pi * (((4 * index[:, None] + 1) * first[None, :]) % 512) / 512
    two = 2 * math.pi * ((index[:, None] * index[None, :]) % 128) / 128
    twist = 2 * math.pi * (((4 * index[:, None] + 1) * index[None, :]) % 65536) / 65536
    c2, s2 = np.cos(two), np.sin(two)
    f32 = np.float32
    e1 = np.concatenate([np.cos(one), -np.sin(one)], 0).astype(f32)
    m2 = np.block([[c2, -s2], [s2, c2]]).astype(f32)
    m3 = np.block([[c2, s2], [-s2, c2]]).astype(f32)
    back = (np.concatenate([np.cos(one).T, -np.sin(one).T], 1) / 16384).astype(f32)
    e1_high, e1_low = split(e1)
    return (
        np.concatenate([e1_high, e1_low], 1),
        np.stack(split(m2)),
        np.stack(split(m3)),
        np.stack(split(back)),
        np.stack([np.cos(twist), -np.sin(twist)]).astype(f32),
    )


def dot(left, right):
    return jnp.dot(left, right, preferred_element_type=F32)


def halves(value):
    high = value.astype(BF16)
    return high, (value - high.astype(F32)).astype(BF16)


def forward(rows, e1, m2, twist):
    parts = []
    for c in range(NC):
        parts.append(
            jnp.concatenate([rows[pl.ds(4 * c + a, NP, stride=16), :] for a in range(4)], 0)
        )
    grid = jnp.concatenate(parts, 1).astype(BF16)
    mixed = dot(e1[...], jnp.concatenate([grid, grid], 0))
    tr, ti = twist[0], twist[1]
    turned = []
    for c in range(NC):
        re, im = mixed[:128, 128 * c : 128 * c + 128], mixed[128:, 128 * c : 128 * c + 128]
        turned.append(jnp.concatenate([re * tr - im * ti, re * ti + im * tr], 1))
    high, low = halves(jnp.concatenate(turned, 0))
    return dot(high, m2[0]) + dot(low, m2[0]) + dot(high, m2[1])


def inverse(spectrum, rows, m3, back, twist):
    high, low = halves(spectrum)
    mixed = dot(high, m3[0]) + dot(low, m3[0]) + dot(high, m3[1])
    tr, ti = twist[0], twist[1]
    turned = []
    for c in range(NC):
        re, im = mixed[128 * c : 128 * c + 128, :128], mixed[128 * c : 128 * c + 128, 128:]
        turned.append(jnp.concatenate([re * tr + im * ti, im * tr - re * ti], 0))
    high, low = halves(jnp.concatenate(turned, 1))
    done = dot(back[0], high) + dot(back[1], high) + dot(back[0], low)
    for c in range(NC):
        for a in range(4):
            rows[pl.ds(a // 2 * 8 + 2 * c + a % 2, NP, stride=16), :] = done[
                NP * a : NP * a + NP, 128 * c : 128 * c + 128
            ]


def product(g, h):
    gr, gi, hr, hi = g[:, :128], g[:, 128:], h[:, :128], h[:, 128:]
    return jnp.concatenate([gr * hr - gi * hi, gr * hi + gi * hr], 1)


def plane_order(k):
    return lax.div(k + 1, 2) * (2 * lax.rem(k, 2) - 1)


def kernel(
    feat, taps, sw, skip, w, e1h, m2h, m3h, bkh, twh, out,
    fv, tv, swv, skv, wv, wr, e1, m2, m3, bk, tw,
    rimsend, rimrecv, cols, f0, gt, f0r, gtr, rows,
    hsend, hrecv, gsend, grecv, csend, crecv, spec, ag, fin, finr,
    lsem, osem, rsem, csem, asem, arem, psem, prem,
):
    me = lax.axis_index("ctx")
    ch = lax.axis_index("ch")
    x, z = lax.rem(me, 4), lax.div(me, 4)
    y, core = lax.div(ch, 2), lax.rem(ch, 2)
    partner = 2 * y + 1 - core
    up, down, across = (2 * lax.rem(y + d, 4) + core for d in (1, 3, 2))
    row = [lax.rem(x + d, 4) for d in range(4)]

    def plane(k):
        return lax.rem(z + 8 + plane_order(k), 8)

    def visit(do, far):
        def one(k, _):
            base = 4 * plane(8 - k if far else k)
            for d in (2, 1, 3, 0):
                do(base + row[d])
            return 0

        def own():
            for d in (2, 1, 3):
                do(4 * z + row[d])

        if not far:
            own()
        lax.fori_loop(1, 8, one, 0)
        if far:
            own()

    local = [
        pltpu.make_async_copy(s, d, lsem.at[i])
        for i, (s, d) in enumerate(
            [(taps, tv), (feat, fv), (sw, swv), (skip, skv), (w, wv), (e1h, e1), (m2h, m2), (twh, tw),
             (m3h, m3), (bkh, bk)]
        )
    ]
    for c in local:
        c.start()

    barrier = pltpu.get_barrier_semaphore()

    def greet(peer):
        for own in (ch, partner):
            pl.semaphore_signal(
                barrier, inc=1, device_id={"ctx": peer, "ch": own}, device_id_type=MESH
            )

    visit(greet, True)
    for other in (partner, up, down, across):
        pl.semaphore_signal(barrier, inc=1, device_id={"ch": other}, device_id_type=MESH)

    local[0].wait()
    for a in range(4):
        rows[pl.ds(a, 128, stride=4), :] = tv[:, 128 * a : 128 * a + 128]
    hsend[...] = rows[...].astype(BF16).reshape(NP, 16, 128)
    hrecv[me] = hsend[me]
    local[1].wait()
    for s in range(3):
        rimsend[pl.ds(8 * s, 8), :] = fv[s, :, 384:].astype(F32).T[120:, :]

    pl.semaphore_wait(barrier, 2 * (NP - 1) + 4)
    rim = pltpu.make_async_remote_copy(
        rimsend, rimrecv, osem.at[3], rsem.at[3],
        device_id={"ctx": lax.rem(me + 1, NP)}, device_id_type=MESH,
    )
    rim.start()

    def spread(send, recv, k, far):
        def one(peer):
            pltpu.make_async_remote_copy(
                send.at[peer], recv.at[me], osem.at[k], rsem.at[k],
                device_id={"ctx": peer}, device_id_type=MESH,
            ).start()

        visit(one, far)

    def arrived(part, sem):
        pltpu.make_async_copy(part, part, sem).wait()

    def mates(i, source, target):
        return pltpu.make_async_remote_copy(
            source, target, psem.at[i], prem.at[i], device_id={"ch": partner}, device_id_type=MESH
        )

    most = pl.ds(0, NP - 1)
    spread(hsend, hrecv, 0, FAR_H)
    local[4].wait()
    swap = [mates(0, wv, wr)]
    swap[0].start()

    local[2].wait()
    local[3].wait()
    cols[...] = jnp.zeros_like(cols)
    for s in range(3):
        for j in range(3):
            cols[pl.ds(3 * s + j, 1), :] = swv[s, pl.ds(j, 1), :]
    cols[pl.ds(9, 1), :] = skv[...]
    col = cols[...].T

    def short(s, edge, width):
        wide = jnp.concatenate([edge, fv[s, :, :width].astype(F32)], 1)
        total = col[:, 3 * s : 3 * s + 1] * wide[:, 128:]
        for j in (1, 2):
            moved = pltpu.roll(wide, j, 1)[:, 128:]
            total = total + col[:, 3 * s + j : 3 * s + j + 1] * moved
        return total

    nothing = jnp.zeros((128, 128), F32)
    gated = short(1, nothing, 512) * short(2, nothing, 512)
    gt[0], gt[1] = gated[:, :256], gated[:, 256:]
    for a in range(1, 4):
        rows[pl.ds(a, 128, stride=4), :] = gated[:, 128 * a : 128 * a + 128]

    rim.wait()
    inside = me > 0

    def edge(s):
        last = jnp.concatenate([jnp.zeros((120, 128), F32), rimrecv[pl.ds(8 * s, 8), :]], 0)
        return jnp.where(inside, last.T, 0.0)

    gt[0, :, :128] = short(1, edge(1), 128) * short(2, edge(2), 128)
    rows[pl.ds(0, 128, stride=4), :] = gt[0, :, :128]
    gsend[...] = rows[...].astype(BF16).reshape(NP, 16, 128)
    grecv[me] = gsend[me]
    spread(gsend, grecv, 1, FAR_G)
    for half in range(2):
        gt[half] = col[:, 9:10] * gt[half]
    whole = short(0, edge(0), 512)
    f0[0], f0[1] = whole[:, :256], whole[:, 256:]
    swap += [mates(1, gt.at[1 - core], gtr), mates(2, f0.at[1 - core], f0r)]
    swap[1].start()
    swap[2].start()

    for c in local[5:]:
        c.wait()
    arrived(hrecv.at[most], rsem.at[0])
    rows[...] = hrecv[...].reshape(512, 128).astype(F32)
    spec[...] = forward(rows, e1, m2, tw)
    for c in swap:
        c.wait_recv()
    arrived(grecv.at[most], rsem.at[1])
    rows[...] = grecv[...].reshape(512, 128).astype(F32)
    inverse(product(forward(rows, e1, m2, tw), spec[...]), rows, m3, bk, tw)

    csend[...] = rows[...].astype(BF16).reshape(NP, 2, 8, 128)
    crecv[core, me] = csend[me, core]

    def half_of(peer, half, sem):
        pltpu.make_async_remote_copy(
            csend.at[peer, half], crecv.at[core, me], sem, csem.at[z],
            device_id={"ctx": peer, "ch": 2 * y + half}, device_id_type=MESH,
        ).start()

    half_of(me, 1 - core, osem.at[4])

    def both_of(peer):
        for half in range(2):
            half_of(peer, half, osem.at[2])

    visit(both_of, FAR_C)

    planes = [lax.rem(z + d, 8) for d in (0, 1, 7, 2, 6, 3, 5, 4)]

    def hand(chip, k, t, other):
        piece = ag.at[pl.ds(2 * chip, 2), pl.ds(pl.multiple_of(16 * planes[k], 16), 16)]
        return pltpu.make_async_remote_copy(
            piece, piece, asem.at[t, k], arem.at[t, k], device_id={"ch": other}, device_id_type=MESH
        )

    sent = []
    for k in (range(7, -1, -1) if FAR_C else range(8)):
        first = planes[k]
        arrived(crecv.at[0, pl.ds(0, 8 if k else 7)], csem.at[first])
        here = pl.ds(pl.multiple_of(16 * first, 16), 16)
        for which, (block, f, g) in enumerate(
            [(core, f0.at[core], gt.at[core]), (1 - core, f0r, gtr)]
        ):
            base = 64 * k + 32 * which
            came = crecv[block, pl.ds(4 * first, 4)].reshape(32, 128)
            rows[pl.ds(base, 32), :] = came.astype(F32)
            for a in range(2):
                lanes = pl.ds(128 * a, 128)
                conv = rows[pl.ds(base + a, 16, stride=2), :]
                ag[2 * y + block, here, lanes] = (
                    f[here, lanes] * (conv + g[here, lanes])
                ).astype(BF16)
        for t, other in ((2, across), (0, up), (1, down)):
            copy = hand(y, k, t, other)
            copy.start()
            sent.append(copy)

    def pair(chip):
        both = ag[pl.ds(2 * chip, 2)].reshape(256, 256)
        columns = pl.ds(pl.multiple_of(256 * chip, 256), 256)
        return dot(jnp.concatenate([wr[:, columns], wv[:, columns]], 0), both)

    total = pair(y)
    for t, other in ((0, down), (1, up), (2, across)):
        for k in range(8):
            hand(other // 2, k, t, other).wait_recv()
        total = total + pair(other // 2)
    fin[...] = total[:128].astype(BF16)
    last = mates(3, fin, finr)
    last.start()
    mine = total[128:].astype(BF16)
    out[:, pl.ds(pl.multiple_of(256 * core, 256), 256)] = mine
    last.wait_recv()
    out[:, pl.ds(pl.multiple_of(256 * (1 - core), 256), 256)] = finr[...]

    for copy in sent + swap + [last]:
        copy.wait_send()
    arrived(hsend.at[most], osem.at[0])
    arrived(gsend.at[most], osem.at[1])
    arrived(csend.at[most], osem.at[2])
    arrived(csend.at[0, 0], osem.at[4])


def local(featurized, short_weights, filter_taps, skip_gain, w_out):
    e1, m2, m3, back, twist = tables()
    far = pl.BlockSpec(memory_space=pl.ANY)
    V = pltpu.VMEM
    chunk = V((NP, 16, 128), BF16)
    two = V((2, 128, 256), F32)
    half = V((128, 256), F32)
    return pl.pallas_call(
        kernel,
        out_shape=jax.ShapeDtypeStruct((128, 512), BF16),
        in_specs=[far] * 10,
        out_specs=pl.BlockSpec(memory_space=pltpu.VMEM),
        scratch_shapes=[
            V((3, 128, 512), BF16), V((128, 512), F32), V((3, 3, 128), F32), V((1, 128), F32),
            V((128, 1024), BF16), V((128, 1024), BF16),
            V(e1.shape, BF16), V(m2.shape, BF16), V(m3.shape, BF16),
            V(back.shape, BF16), V(twist.shape, F32),
            V((24, 128), F32), V((24, 128), F32), V((128, 128), F32),
            two, two, half, half, V((512, 128), F32), chunk, chunk, chunk, chunk,
            V((NP, 2, 8, 128), BF16), V((2, NP, 8, 128), BF16),
            V((512, 256), F32), V((8, 128, 256), BF16), V((128, 256), BF16), V((128, 256), BF16),
            pltpu.SemaphoreType.DMA((10,)),
            pltpu.SemaphoreType.DMA((5,)),
            pltpu.SemaphoreType.DMA((4,)),
            pltpu.SemaphoreType.DMA((8,)),
            pltpu.SemaphoreType.DMA((3, 8)),
            pltpu.SemaphoreType.DMA((3, 8)),
            pltpu.SemaphoreType.DMA((4,)),
            pltpu.SemaphoreType.DMA((4,)),
        ],
        compiler_params=pltpu.CompilerParams(collective_id=0, has_side_effects=True),
        name="hyena",
    )(
        featurized, filter_taps, jnp.swapaxes(short_weights, 1, 2), skip_gain.reshape(1, 128),
        w_out, e1, m2, m3, back, twist,
    )


def solution(mesh):
    in_specs = (P(None, "ch", "ctx"), P(None, "ch", None), P("ch", "ctx"), P("ch"), P("ch", None))
    out_specs = P("ch", "ctx")
    return jax.shard_map(local, mesh=mesh, in_specs=in_specs, out_specs=out_specs, check_vma=False)
```

```python
import math

import jax
import jax.numpy as jnp
import numpy as np
from jax import lax
from jax.experimental import pallas as pl
from jax.experimental.pallas import tpu as pltpu
from jax.sharding import PartitionSpec as P

NP = 32
NC = 4
RELAYED, LAG = 6, 8
MESH = pl.DeviceIdType.MESH
F32 = jnp.float32
BF16 = jnp.bfloat16


def split(table):
    high = table.astype(BF16)
    return high, (table - high.astype(np.float32)).astype(BF16)


def tables():
    index = np.arange(128)
    first = 4 * (index % NP) + index // NP
    one = 2 * math.pi * (((4 * index[:, None] + 1) * first[None, :]) % 512) / 512
    two = 2 * math.pi * ((index[:, None] * index[None, :]) % 128) / 128
    twist = 2 * math.pi * (((4 * index[:, None] + 1) * index[None, :]) % 65536) / 65536
    c2, s2 = np.cos(two), np.sin(two)
    f32 = np.float32
    e1 = np.concatenate([np.cos(one), -np.sin(one)], 0).astype(f32)
    m2 = np.block([[c2, -s2], [s2, c2]]).astype(f32)
    m3 = np.block([[c2, s2], [-s2, c2]]).astype(f32)
    back = (np.concatenate([np.cos(one).T, -np.sin(one).T], 1) / 16384).astype(f32)
    e1_high, e1_low = split(e1)
    return (
        np.concatenate([e1_high, e1_low], 1),
        np.stack(split(m2)),
        np.stack(split(m3)),
        np.stack(split(back)),
        np.stack([np.cos(twist), -np.sin(twist)]).astype(f32),
    )


def dot(left, right):
    return jnp.dot(left, right, preferred_element_type=F32)


def halves(value):
    high = value.astype(BF16)
    return high, (value - high.astype(F32)).astype(BF16)


def forward(rows, e1, m2, twist):
    parts = []
    for c in range(NC):
        parts.append(
            jnp.concatenate([rows[pl.ds(4 * c + a, NP, stride=16), :] for a in range(4)], 0)
        )
    grid = jnp.concatenate(parts, 1).astype(BF16)
    mixed = dot(e1[...], jnp.concatenate([grid, grid], 0))
    tr, ti = twist[0], twist[1]
    turned = []
    for c in range(NC):
        re, im = mixed[:128, 128 * c : 128 * c + 128], mixed[128:, 128 * c : 128 * c + 128]
        turned.append(jnp.concatenate([re * tr - im * ti, re * ti + im * tr], 1))
    high, low = halves(jnp.concatenate(turned, 0))
    return dot(high, m2[0]) + dot(low, m2[0]) + dot(high, m2[1])


def inverse(spectrum, rows, m3, back, twist):
    high, low = halves(spectrum)
    mixed = dot(high, m3[0]) + dot(low, m3[0]) + dot(high, m3[1])
    tr, ti = twist[0], twist[1]
    turned = []
    for c in range(NC):
        re, im = mixed[128 * c : 128 * c + 128, :128], mixed[128 * c : 128 * c + 128, 128:]
        turned.append(jnp.concatenate([re * tr + im * ti, im * tr - re * ti], 0))
    high, low = halves(jnp.concatenate(turned, 1))
    done = dot(back[0], high) + dot(back[1], high) + dot(back[0], low)
    for c in range(NC):
        for a in range(4):
            rows[pl.ds(a // 2 * 8 + 2 * c + a % 2, NP, stride=16), :] = done[
                NP * a : NP * a + NP, 128 * c : 128 * c + 128
            ]


def product(g, h):
    gr, gi, hr, hi = g[:, :128], g[:, 128:], h[:, :128], h[:, 128:]
    return jnp.concatenate([gr * hr - gi * hi, gr * hi + gi * hr], 1)


def plane_order(k):
    return lax.div(k + 1, 2) * (2 * lax.rem(k, 2) - 1)


def kernel(
    feat, taps, sw, skip, w, e1h, m2h, m3h, bkh, twh, out,
    fv, tv, swv, skv, wv, wr, e1, m2, m3, bk, tw,
    rimsend, rimrecv, cols, f0, gt, f0r, gtr, rows,
    hsend, hrecv, gsend, grecv, csend, crecv, spec, ag, fin, finr,
    lsem, osem, rsem, csem, asem, arem, psem, prem,
):
    me = lax.axis_index("ctx")
    ch = lax.axis_index("ch")
    x, z = lax.rem(me, 4), lax.div(me, 4)
    y, core = lax.div(ch, 2), lax.rem(ch, 2)
    partner = 2 * y + 1 - core
    up, down, across = (2 * lax.rem(y + d, 4) + core for d in (1, 3, 2))
    row = [lax.rem(x + d, 4) for d in range(4)]

    def plane(k):
        return lax.rem(z + 8 + plane_order(k), 8)

    def visit(do, far):
        def one(k, _):
            base = 4 * plane(8 - k if far else k)
            for d in (2, 1, 3, 0):
                do(base + row[d])
            return 0

        def own():
            for d in (2, 1, 3):
                do(4 * z + row[d])

        if not far:
            own()
        lax.fori_loop(1, 8, one, 0)
        if far:
            own()

    local = [
        pltpu.make_async_copy(s, d, lsem.at[i])
        for i, (s, d) in enumerate(
            [(taps, tv), (feat, fv), (sw, swv), (skip, skv), (w, wv), (e1h, e1), (m2h, m2), (twh, tw),
             (m3h, m3), (bkh, bk)]
        )
    ]
    barrier = pltpu.get_barrier_semaphore()

    def greet(peer):
        for own in (ch, partner):
            pl.semaphore_signal(
                barrier, inc=1, device_id={"ctx": peer, "ch": own}, device_id_type=MESH
            )

    visit(greet, True)
    for other in (partner, up, down, across):
        pl.semaphore_signal(barrier, inc=1, device_id={"ch": other}, device_id_type=MESH)
    for c in local:
        c.start()

    local[0].wait()
    for a in range(4):
        rows[pl.ds(a, 128, stride=4), :] = tv[:, 128 * a : 128 * a + 128]
    hsend[...] = rows[...].astype(BF16).reshape(NP, 16, 128)
    hrecv[me] = hsend[me]
    local[1].wait()
    for s in range(3):
        rimsend[pl.ds(8 * s, 8), :] = fv[s, :, 384:].astype(F32).T[120:, :]

    pl.semaphore_wait(barrier, 2 * (NP - 1) + 4)
    rim = pltpu.make_async_remote_copy(
        rimsend, rimrecv, osem.at[3], rsem.at[3],
        device_id={"ctx": lax.rem(me + 1, NP)}, device_id_type=MESH,
    )
    rim.start()

    def spread(send, recv, k, far):
        def one(peer):
            pltpu.make_async_remote_copy(
                send.at[peer], recv.at[me], osem.at[k], rsem.at[k],
                device_id={"ctx": peer}, device_id_type=MESH,
            ).start()

        visit(one, far)

    def arrived(part, sem):
        pltpu.make_async_copy(part, part, sem).wait()

    def mates(i, source, target):
        return pltpu.make_async_remote_copy(
            source, target, psem.at[i], prem.at[i], device_id={"ch": partner}, device_id_type=MESH
        )

    most = pl.ds(0, NP - 1)
    spread(hsend, hrecv, 0, False)
    local[4].wait()
    swap = [mates(0, wv, wr)]
    swap[0].start()

    local[2].wait()
    local[3].wait()
    cols[...] = jnp.zeros_like(cols)
    for s in range(3):
        for j in range(3):
            cols[pl.ds(3 * s + j, 1), :] = swv[s, pl.ds(j, 1), :]
    cols[pl.ds(9, 1), :] = skv[...]
    col = cols[...].T

    def short(s, edge, width):
        wide = jnp.concatenate([edge, fv[s, :, :width].astype(F32)], 1)
        total = col[:, 3 * s : 3 * s + 1] * wide[:, 128:]
        for j in (1, 2):
            moved = pltpu.roll(wide, j, 1)[:, 128:]
            total = total + col[:, 3 * s + j : 3 * s + j + 1] * moved
        return total

    nothing = jnp.zeros((128, 128), F32)
    gated = short(1, nothing, 512) * short(2, nothing, 512)
    gt[0], gt[1] = gated[:, :256], gated[:, 256:]
    for a in range(1, 4):
        rows[pl.ds(a, 128, stride=4), :] = gated[:, 128 * a : 128 * a + 128]

    rim.wait()
    inside = me > 0

    def edge(s):
        last = jnp.concatenate([jnp.zeros((120, 128), F32), rimrecv[pl.ds(8 * s, 8), :]], 0)
        return jnp.where(inside, last.T, 0.0)

    gt[0, :, :128] = short(1, edge(1), 128) * short(2, edge(2), 128)
    rows[pl.ds(0, 128, stride=4), :] = gt[0, :, :128]
    gsend[...] = rows[...].astype(BF16).reshape(NP, 16, 128)
    grecv[me] = gsend[me]
    spread(gsend, grecv, 1, True)
    for half in range(2):
        gt[half] = col[:, 9:10] * gt[half]
    whole = short(0, edge(0), 512)
    f0[0], f0[1] = whole[:, :256], whole[:, 256:]
    swap += [mates(1, gt.at[1 - core], gtr), mates(2, f0.at[1 - core], f0r)]
    swap[1].start()
    swap[2].start()

    for c in local[5:]:
        c.wait()
    arrived(hrecv.at[most], rsem.at[0])
    rows[...] = hrecv[...].reshape(512, 128).astype(F32)
    spec[...] = forward(rows, e1, m2, tw)
    for c in swap:
        c.wait_recv()
    arrived(grecv.at[most], rsem.at[1])
    rows[...] = grecv[...].reshape(512, 128).astype(F32)
    inverse(product(forward(rows, e1, m2, tw), spec[...]), rows, m3, bk, tw)

    csend[...] = rows[...].astype(BF16).reshape(NP, 2, 8, 128)
    crecv[core, me] = csend[me, core]

    def half_of(peer, half, sem):
        pltpu.make_async_remote_copy(
            csend.at[peer, half], crecv.at[core, me], sem, csem.at[z],
            device_id={"ctx": peer, "ch": 2 * y + half}, device_id_type=MESH,
        ).start()

    half_of(me, 1 - core, osem.at[4])

    def both_of(peer):
        for half in range(2):
            half_of(peer, half, osem.at[2])

    visit(both_of, False)

    planes = [lax.rem(z + d, 8) for d in (0, 1, 7, 2, 6, 3, 5, 4)]

    def hand(chip, k, t, other):
        piece = ag.at[pl.ds(2 * chip, 2), pl.ds(pl.multiple_of(16 * planes[k], 16), 16)]
        return pltpu.make_async_remote_copy(
            piece, piece, asem.at[t, k], arem.at[t, k], device_id={"ch": other}, device_id_type=MESH
        )

    sent = []

    def go(*args):
        copy = hand(*args)
        copy.start()
        sent.append(copy)

    def own(k):
        first = planes[k]
        arrived(crecv.at[0, pl.ds(0, 8 if k else 7)], csem.at[first])
        here = pl.ds(pl.multiple_of(16 * first, 16), 16)
        for which, (block, f, g) in enumerate(
            [(core, f0.at[core], gt.at[core]), (1 - core, f0r, gtr)]
        ):
            base = 64 * k + 32 * which
            came = crecv[block, pl.ds(4 * first, 4)].reshape(32, 128)
            rows[pl.ds(base, 32), :] = came.astype(F32)
            for a in range(2):
                lanes = pl.ds(128 * a, 128)
                conv = rows[pl.ds(base + a, 16, stride=2), :]
                ag[2 * y + block, here, lanes] = (
                    f[here, lanes] * (conv + g[here, lanes])
                ).astype(BF16)
        if k >= RELAYED:
            go(y, k, 2, across)
        go(y, k, k % 2, (up, down)[k % 2])
        go(y, k, 1 - k % 2, (down, up)[k % 2])

    taken = set()

    def take(t, k):
        if (t, k) not in taken:
            taken.add((t, k))
            other = (down, up, across)[t]
            hand(lax.div(other, 2), k, t, other).wait_recv()

    def relay(k):
        take(k % 2, k)
        go(lax.div((down, up)[k % 2], 2), k, 2, (up, down)[k % 2])

    for step in range(8 + LAG):
        if step < 8:
            own(step)
        if 0 <= step - LAG < RELAYED:
            relay(step - LAG)

    def pair(chip):
        both = ag[pl.ds(2 * chip, 2)].reshape(256, 256)
        columns = pl.ds(pl.multiple_of(256 * chip, 256), 256)
        return dot(wr[:, columns], both), dot(wv[:, columns], both)

    theirs, mine = pair(y)
    for t, other in ((0, down), (1, up), (2, across)):
        for k in range(8):
            take(t, k)
        more = pair(lax.div(other, 2))
        theirs, mine = theirs + more[0], mine + more[1]
    fin[...] = theirs.astype(BF16)
    last = mates(3, fin, finr)
    last.start()
    out[:, pl.ds(pl.multiple_of(256 * core, 256), 256)] = mine.astype(BF16)
    last.wait_recv()
    out[:, pl.ds(pl.multiple_of(256 * (1 - core), 256), 256)] = finr[...]

    for copy in sent + swap + [last]:
        copy.wait_send()
    arrived(hsend.at[most], osem.at[0])
    arrived(gsend.at[most], osem.at[1])
    arrived(csend.at[most], osem.at[2])
    arrived(csend.at[0, 0], osem.at[4])


def local(featurized, short_weights, filter_taps, skip_gain, w_out):
    e1, m2, m3, back, twist = tables()
    far = pl.BlockSpec(memory_space=pl.ANY)
    V = pltpu.VMEM
    chunk = V((NP, 16, 128), BF16)
    two = V((2, 128, 256), F32)
    half = V((128, 256), F32)
    return pl.pallas_call(
        kernel,
        out_shape=jax.ShapeDtypeStruct((128, 512), BF16),
        in_specs=[far] * 10,
        out_specs=pl.BlockSpec(memory_space=pltpu.VMEM),
        scratch_shapes=[
            V((3, 128, 512), BF16), V((128, 512), F32), V((3, 3, 128), F32), V((1, 128), F32),
            V((128, 1024), BF16), V((128, 1024), BF16),
            V(e1.shape, BF16), V(m2.shape, BF16), V(m3.shape, BF16),
            V(back.shape, BF16), V(twist.shape, F32),
            V((24, 128), F32), V((24, 128), F32), V((128, 128), F32),
            two, two, half, half, V((512, 128), F32), chunk, chunk, chunk, chunk,
            V((NP, 2, 8, 128), BF16), V((2, NP, 8, 128), BF16),
            V((512, 256), F32), V((8, 128, 256), BF16), V((128, 256), BF16), V((128, 256), BF16),
            pltpu.SemaphoreType.DMA((10,)),
            pltpu.SemaphoreType.DMA((5,)),
            pltpu.SemaphoreType.DMA((4,)),
            pltpu.SemaphoreType.DMA((8,)),
            pltpu.SemaphoreType.DMA((3, 8)),
            pltpu.SemaphoreType.DMA((3, 8)),
            pltpu.SemaphoreType.DMA((4,)),
            pltpu.SemaphoreType.DMA((4,)),
        ],
        compiler_params=pltpu.CompilerParams(collective_id=0, has_side_effects=True),
        name="hyena",
    )(
        featurized, filter_taps, jnp.swapaxes(short_weights, 1, 2), skip_gain.reshape(1, 128),
        w_out, e1, m2, m3, back, twist,
    )


def solution(mesh):
    in_specs = (P(None, "ch", "ctx"), P(None, "ch", None), P("ch", "ctx"), P("ch"), P("ch", None))
    out_specs = P("ch", "ctx")
    return jax.shard_map(local, mesh=mesh, in_specs=in_specs, out_specs=out_specs, check_vma=False)
```

```python
import math

import jax
import jax.numpy as jnp
import numpy as np
from jax import lax
from jax.experimental import pallas as pl
from jax.experimental.pallas import tpu as pltpu
from jax.sharding import PartitionSpec as P

NP = 32
NC = 4
RELAYED, LAG = 6, 6
MESH = pl.DeviceIdType.MESH
F32 = jnp.float32
BF16 = jnp.bfloat16


def split(table):
    high = table.astype(BF16)
    return high, (table - high.astype(np.float32)).astype(BF16)


def tables():
    index = np.arange(128)
    first = 4 * (index % NP) + index // NP
    one = 2 * math.pi * (((4 * index[:, None] + 1) * first[None, :]) % 512) / 512
    two = 2 * math.pi * ((index[:, None] * index[None, :]) % 128) / 128
    twist = 2 * math.pi * (((4 * index[:, None] + 1) * index[None, :]) % 65536) / 65536
    c2, s2 = np.cos(two), np.sin(two)
    f32 = np.float32
    e1 = np.concatenate([np.cos(one), -np.sin(one)], 0).astype(f32)
    m2 = np.block([[c2, -s2], [s2, c2]]).astype(f32)
    m3 = np.block([[c2, s2], [-s2, c2]]).astype(f32)
    back = (np.concatenate([np.cos(one).T, -np.sin(one).T], 1) / 16384).astype(f32)
    e1_high, e1_low = split(e1)
    return (
        np.concatenate([e1_high, e1_low], 1),
        np.stack(split(m2)),
        np.stack(split(m3)),
        np.stack(split(back)),
        np.stack([np.cos(twist), -np.sin(twist)]).astype(f32),
    )


def dot(left, right):
    return jnp.dot(left, right, preferred_element_type=F32)


def halves(value):
    high = value.astype(BF16)
    return high, (value - high.astype(F32)).astype(BF16)


def forward(rows, e1, m2, twist):
    parts = []
    for c in range(NC):
        parts.append(
            jnp.concatenate([rows[pl.ds(4 * c + a, NP, stride=16), :] for a in range(4)], 0)
        )
    grid = jnp.concatenate(parts, 1).astype(BF16)
    mixed = dot(e1[...], jnp.concatenate([grid, grid], 0))
    tr, ti = twist[0], twist[1]
    turned = []
    for c in range(NC):
        re, im = mixed[:128, 128 * c : 128 * c + 128], mixed[128:, 128 * c : 128 * c + 128]
        turned.append(jnp.concatenate([re * tr - im * ti, re * ti + im * tr], 1))
    high, low = halves(jnp.concatenate(turned, 0))
    return dot(high, m2[0]) + dot(low, m2[0]) + dot(high, m2[1])


def inverse(spectrum, rows, m3, back, twist):
    high, low = halves(spectrum)
    mixed = dot(high, m3[0]) + dot(low, m3[0]) + dot(high, m3[1])
    tr, ti = twist[0], twist[1]
    turned = []
    for c in range(NC):
        re, im = mixed[128 * c : 128 * c + 128, :128], mixed[128 * c : 128 * c + 128, 128:]
        turned.append(jnp.concatenate([re * tr + im * ti, im * tr - re * ti], 0))
    high, low = halves(jnp.concatenate(turned, 1))
    done = dot(back[0], high) + dot(back[1], high) + dot(back[0], low)
    for c in range(NC):
        for a in range(4):
            rows[pl.ds(4 * c + a, NP, stride=16), :] = done[
                NP * a : NP * a + NP, 128 * c : 128 * c + 128
            ]


def product(g, h):
    gr, gi, hr, hi = g[:, :128], g[:, 128:], h[:, :128], h[:, 128:]
    return jnp.concatenate([gr * hr - gi * hi, gr * hi + gi * hr], 1)


def plane_order(k):
    return lax.div(k + 1, 2) * (2 * lax.rem(k, 2) - 1)


def kernel(
    feat, taps, sw, skip, w, e1h, m2h, m3h, bkh, twh, out,
    fv, tv, swv, skv, wv, wr, e1, m2, m3, bk, tw,
    rimsend, rimrecv, cols, f0, gt, rows,
    hsend, hrecv, gsend, grecv, csend, crecv, spec, ag, fin, finr,
    lsem, osem, rsem, csem, asem, arem, psem, prem,
):
    me = lax.axis_index("ctx")
    ch = lax.axis_index("ch")
    x, z = lax.rem(me, 4), lax.div(me, 4)
    y, core = lax.div(ch, 2), lax.rem(ch, 2)
    partner = 2 * y + 1 - core
    up, down, across = (2 * lax.rem(y + d, 4) + core for d in (1, 3, 2))
    row = [lax.rem(x + d, 4) for d in range(4)]

    def plane(k):
        return lax.rem(z + 8 + plane_order(k), 8)

    def visit(do, far):
        def one(k, _):
            base = 4 * plane(8 - k if far else k)
            for d in (2, 1, 3, 0):
                do(base + row[d])
            return 0

        def own():
            for d in (2, 1, 3):
                do(4 * z + row[d])

        if not far:
            own()
        lax.fori_loop(1, 8, one, 0)
        if far:
            own()

    local = [
        pltpu.make_async_copy(s, d, lsem.at[i])
        for i, (s, d) in enumerate(
            [(taps, tv), (feat, fv), (sw, swv), (skip, skv), (w, wv), (e1h, e1), (m2h, m2), (twh, tw),
             (m3h, m3), (bkh, bk)]
        )
    ]
    barrier = pltpu.get_barrier_semaphore()

    def greet(peer):
        pl.semaphore_signal(barrier, inc=1, device_id={"ctx": peer}, device_id_type=MESH)

    visit(greet, True)
    for other in (partner, up, down, across):
        pl.semaphore_signal(barrier, inc=1, device_id={"ch": other}, device_id_type=MESH)
    for c in local:
        c.start()

    local[0].wait()
    for a in range(4):
        rows[pl.ds(a, 128, stride=4), :] = tv[:, 128 * a : 128 * a + 128]
    hsend[...] = rows[...].astype(BF16).reshape(NP, 16, 128)
    hrecv[me] = hsend[me]
    local[1].wait()
    for s in range(3):
        rimsend[pl.ds(8 * s, 8), :] = fv[s, :, 384:].astype(F32).T[120:, :]

    pl.semaphore_wait(barrier, NP - 1 + 4)
    rim = pltpu.make_async_remote_copy(
        rimsend, rimrecv, osem.at[3], rsem.at[3],
        device_id={"ctx": lax.rem(me + 1, NP)}, device_id_type=MESH,
    )
    rim.start()

    def spread(send, recv, k, sem, far):
        def one(peer):
            pltpu.make_async_remote_copy(
                send.at[peer], recv.at[me], osem.at[k], sem,
                device_id={"ctx": peer}, device_id_type=MESH,
            ).start()

        visit(one, far)

    def arrived(part, sem):
        pltpu.make_async_copy(part, part, sem).wait()

    def mates(i, source, target):
        return pltpu.make_async_remote_copy(
            source, target, psem.at[i], prem.at[i], device_id={"ch": partner}, device_id_type=MESH
        )

    most = pl.ds(0, NP - 1)
    spread(hsend, hrecv, 0, rsem.at[0], False)
    local[4].wait()
    swap = mates(0, wv, wr)
    swap.start()

    local[2].wait()
    local[3].wait()
    cols[...] = jnp.zeros_like(cols)
    for s in range(3):
        for j in range(3):
            cols[pl.ds(3 * s + j, 1), :] = swv[s, pl.ds(j, 1), :]
    cols[pl.ds(9, 1), :] = skv[...]
    col = cols[...].T

    def short(s, edge, width):
        wide = jnp.concatenate([edge, fv[s, :, :width].astype(F32)], 1)
        total = col[:, 3 * s : 3 * s + 1] * wide[:, 128:]
        for j in (1, 2):
            moved = pltpu.roll(wide, j, 1)[:, 128:]
            total = total + col[:, 3 * s + j : 3 * s + j + 1] * moved
        return total

    nothing = jnp.zeros((128, 128), F32)
    gt[...] = short(1, nothing, 512) * short(2, nothing, 512)
    for a in range(1, 4):
        rows[pl.ds(a, 128, stride=4), :] = gt[:, 128 * a : 128 * a + 128]

    rim.wait()
    inside = me > 0

    def edge(s):
        last = jnp.concatenate([jnp.zeros((120, 128), F32), rimrecv[pl.ds(8 * s, 8), :]], 0)
        return jnp.where(inside, last.T, 0.0)

    gt[:, :128] = short(1, edge(1), 128) * short(2, edge(2), 128)
    rows[pl.ds(0, 128, stride=4), :] = gt[:, :128]
    gsend[...] = rows[...].astype(BF16).reshape(NP, 16, 128)
    grecv[me] = gsend[me]
    spread(gsend, grecv, 1, rsem.at[1], True)
    gt[...] = col[:, 9:10] * gt[...]
    f0[...] = short(0, edge(0), 512)

    for c in local[5:]:
        c.wait()
    arrived(hrecv.at[most], rsem.at[0])
    rows[...] = hrecv[...].reshape(512, 128).astype(F32)
    spec[...] = forward(rows, e1, m2, tw)
    swap.wait_recv()
    arrived(grecv.at[most], rsem.at[1])
    rows[...] = grecv[...].reshape(512, 128).astype(F32)
    inverse(product(forward(rows, e1, m2, tw), spec[...]), rows, m3, bk, tw)

    csend[...] = rows[...].astype(BF16).reshape(NP, 16, 128)
    crecv[me] = csend[me]
    spread(csend, crecv, 2, csem.at[z], False)

    planes = [lax.rem(z + d, 8) for d in (0, 1, 7, 2, 6, 3, 5, 4)]

    def hand(chip, k, t, other):
        piece = ag.at[chip, pl.ds(pl.multiple_of(16 * planes[k], 16), 16)]
        return pltpu.make_async_remote_copy(
            piece, piece, asem.at[t, k], arem.at[t, k], device_id={"ch": other}, device_id_type=MESH
        )

    sent = []

    def go(*args):
        copy = hand(*args)
        copy.start()
        sent.append(copy)

    def own(k):
        first = planes[k]
        arrived(crecv.at[pl.ds(0, 4 if k else 3)], csem.at[first])
        here = pl.ds(pl.multiple_of(16 * first, 16), 16)
        came = crecv[pl.ds(4 * first, 4)].reshape(64, 128)
        rows[pl.ds(64 * k, 64), :] = came.astype(F32)
        for a in range(4):
            lanes = pl.ds(128 * a, 128)
            conv = rows[pl.ds(64 * k + a, 16, stride=4), :]
            ag[y, here, lanes] = (f0[here, lanes] * (conv + gt[here, lanes])).astype(BF16)
        if k >= RELAYED:
            go(y, k, 2, across)
        go(y, k, k % 2, (up, down)[k % 2])
        go(y, k, 1 - k % 2, (down, up)[k % 2])

    taken = set()

    def take(t, k):
        if (t, k) not in taken:
            taken.add((t, k))
            other = (down, up, across)[t]
            hand(lax.div(other, 2), k, t, other).wait_recv()

    def relay(k):
        take(k % 2, k)
        go(lax.div((down, up)[k % 2], 2), k, 2, (up, down)[k % 2])

    for step in range(8 + LAG):
        if step < 8:
            own(step)
        if 0 <= step - LAG < RELAYED:
            relay(step - LAG)

    def term(chip):
        columns = pl.ds(pl.multiple_of(256 * chip + 128 * core, 128), 128)
        return dot(wr[:, columns], ag[chip]), dot(wv[:, columns], ag[chip])

    theirs, mine = term(y)
    for t, other in ((0, down), (1, up), (2, across)):
        for k in range(8):
            take(t, k)
        more = term(lax.div(other, 2))
        theirs, mine = theirs + more[0], mine + more[1]
    fin[...] = theirs
    last = mates(1, fin, finr)
    last.start()
    last.wait_recv()
    out[...] = (mine + finr[...]).astype(BF16)

    for copy in sent + [swap, last]:
        copy.wait_send()
    arrived(hsend.at[most], osem.at[0])
    arrived(gsend.at[most], osem.at[1])
    arrived(csend.at[most], osem.at[2])


def local(featurized, short_weights, filter_taps, skip_gain, w_out):
    e1, m2, m3, back, twist = tables()
    far = pl.BlockSpec(memory_space=pl.ANY)
    V = pltpu.VMEM
    chunk = V((NP, 16, 128), BF16)
    block = V((128, 512), F32)
    return pl.pallas_call(
        kernel,
        out_shape=jax.ShapeDtypeStruct((128, 512), BF16),
        in_specs=[far] * 10,
        out_specs=pl.BlockSpec(memory_space=pltpu.VMEM),
        scratch_shapes=[
            V((3, 128, 512), BF16), V((128, 512), F32), V((3, 3, 128), F32), V((1, 128), F32),
            V((128, 1024), BF16), V((128, 1024), BF16),
            V(e1.shape, BF16), V(m2.shape, BF16), V(m3.shape, BF16),
            V(back.shape, BF16), V(twist.shape, F32),
            V((24, 128), F32), V((24, 128), F32), V((128, 128), F32),
            block, block, V((512, 128), F32), chunk, chunk, chunk, chunk,
            chunk, chunk,
            V((512, 256), F32), V((4, 128, 512), BF16), block, block,
            pltpu.SemaphoreType.DMA((10,)),
            pltpu.SemaphoreType.DMA((4,)),
            pltpu.SemaphoreType.DMA((4,)),
            pltpu.SemaphoreType.DMA((8,)),
            pltpu.SemaphoreType.DMA((3, 8)),
            pltpu.SemaphoreType.DMA((3, 8)),
            pltpu.SemaphoreType.DMA((2,)),
            pltpu.SemaphoreType.DMA((2,)),
        ],
        compiler_params=pltpu.CompilerParams(collective_id=0, has_side_effects=True),
        name="hyena",
    )(
        featurized, filter_taps, jnp.swapaxes(short_weights, 1, 2), skip_gain.reshape(1, 128),
        w_out, e1, m2, m3, back, twist,
    )


def solution(mesh):
    in_specs = (P(None, "ch", "ctx"), P(None, "ch", None), P("ch", "ctx"), P("ch"), P("ch", None))
    out_specs = P("ch", "ctx")
    return jax.shard_map(local, mesh=mesh, in_specs=in_specs, out_specs=out_specs, check_vma=False)
```

```python
import math

import jax
import jax.numpy as jnp
import numpy as np
from jax import lax
from jax.experimental import pallas as pl
from jax.experimental.pallas import tpu as pltpu
from jax.sharding import PartitionSpec as P

NP = 32
NC = 4
RELAYED, LAG = 6, 6
MESH = pl.DeviceIdType.MESH
F32 = jnp.float32
BF16 = jnp.bfloat16


def split(table):
    high = table.astype(BF16)
    return high, (table - high.astype(np.float32)).astype(BF16)


def tables():
    index = np.arange(128)
    first = 4 * (index % NP) + index // NP
    one = 2 * math.pi * (((4 * index[:, None] + 1) * first[None, :]) % 512) / 512
    two = 2 * math.pi * ((index[:, None] * index[None, :]) % 128) / 128
    twist = 2 * math.pi * (((4 * index[:, None] + 1) * index[None, :]) % 65536) / 65536
    c2, s2 = np.cos(two), np.sin(two)
    f32 = np.float32
    e1 = np.concatenate([np.cos(one), -np.sin(one)], 0).astype(f32)
    m2 = np.block([[c2, -s2], [s2, c2]]).astype(f32)
    m3 = np.block([[c2, s2], [-s2, c2]]).astype(f32)
    back = (np.concatenate([np.cos(one).T, -np.sin(one).T], 1) / 16384).astype(f32)
    e1_high, e1_low = split(e1)
    return (
        np.concatenate([e1_high, e1_low], 1),
        np.stack(split(m2)),
        np.stack(split(m3)),
        np.stack(split(back)),
        np.stack([np.cos(twist), -np.sin(twist)]).astype(f32),
    )


def dot(left, right):
    return jnp.dot(left, right, preferred_element_type=F32)


def halves(value):
    high = value.astype(BF16)
    return high, (value - high.astype(F32)).astype(BF16)


def forward(rows, e1, m2, twist):
    parts = []
    for c in range(NC):
        parts.append(
            jnp.concatenate([rows[pl.ds(4 * c + a, NP, stride=16), :] for a in range(4)], 0)
        )
    grid = jnp.concatenate(parts, 1).astype(BF16)
    mixed = dot(e1[...], jnp.concatenate([grid, grid], 0))
    tr, ti = twist[0], twist[1]
    turned = []
    for c in range(NC):
        re, im = mixed[:128, 128 * c : 128 * c + 128], mixed[128:, 128 * c : 128 * c + 128]
        turned.append(jnp.concatenate([re * tr - im * ti, re * ti + im * tr], 1))
    high, low = halves(jnp.concatenate(turned, 0))
    return dot(jnp.concatenate([high, low, high], 1), jnp.concatenate([m2[0], m2[0], m2[1]], 0))


def inverse(spectrum, rows, m3, back, twist):
    high, low = halves(spectrum)
    mixed = dot(jnp.concatenate([high, low, high], 1), jnp.concatenate([m3[0], m3[0], m3[1]], 0))
    tr, ti = twist[0], twist[1]
    turned = []
    for c in range(NC):
        re, im = mixed[128 * c : 128 * c + 128, :128], mixed[128 * c : 128 * c + 128, 128:]
        turned.append(jnp.concatenate([re * tr + im * ti, im * tr - re * ti], 0))
    high, low = halves(jnp.concatenate(turned, 1))
    done = dot(jnp.concatenate([back[0], back[1], back[0]], 1), jnp.concatenate([high, high, low], 0))
    for c in range(NC):
        for a in range(4):
            rows[pl.ds(4 * c + a, NP, stride=16), :] = done[
                NP * a : NP * a + NP, 128 * c : 128 * c + 128
            ]


def product(g, h):
    gr, gi, hr, hi = g[:, :128], g[:, 128:], h[:, :128], h[:, 128:]
    return jnp.concatenate([gr * hr - gi * hi, gr * hi + gi * hr], 1)


def plane_order(k):
    return lax.div(k + 1, 2) * (2 * lax.rem(k, 2) - 1)


def kernel(
    feat, taps, sw, skip, w, e1h, m2h, m3h, bkh, twh, out,
    fv, tv, swv, skv, wv, wr, e1, m2, m3, bk, tw,
    rimsend, rimrecv, cols, f0, gt, rows,
    hsend, hrecv, gsend, grecv, csend, crecv, spec, ag, fin, finr,
    lsem, osem, rsem, csem, asem, arem, psem, prem,
):
    me = lax.axis_index("ctx")
    ch = lax.axis_index("ch")
    x, z = lax.rem(me, 4), lax.div(me, 4)
    y, core = lax.div(ch, 2), lax.rem(ch, 2)
    partner = 2 * y + 1 - core
    up, down, across = (2 * lax.rem(y + d, 4) + core for d in (1, 3, 2))
    row = [lax.rem(x + d, 4) for d in range(4)]

    def plane(k):
        return lax.rem(z + 8 + plane_order(k), 8)

    def visit(do, far):
        def one(k, _):
            base = 4 * plane(8 - k if far else k)
            for d in (2, 1, 3, 0):
                do(base + row[d])
            return 0

        def own():
            for d in (2, 1, 3):
                do(4 * z + row[d])

        if not far:
            own()
        lax.fori_loop(1, 8, one, 0)
        if far:
            own()

    local = [
        pltpu.make_async_copy(s, d, lsem.at[i])
        for i, (s, d) in enumerate(
            [(taps, tv), (feat, fv), (sw, swv), (skip, skv), (w, wv), (e1h, e1), (m2h, m2), (twh, tw),
             (m3h, m3), (bkh, bk)]
        )
    ]
    barrier = pltpu.get_barrier_semaphore()

    def greet(peer):
        pl.semaphore_signal(barrier, inc=1, device_id={"ctx": peer}, device_id_type=MESH)

    visit(greet, True)
    for other in (partner, up, down, across):
        pl.semaphore_signal(barrier, inc=1, device_id={"ch": other}, device_id_type=MESH)
    for c in local:
        c.start()

    local[0].wait()
    for a in range(4):
        rows[pl.ds(a, 128, stride=4), :] = tv[:, 128 * a : 128 * a + 128]
    hsend[...] = rows[...].astype(BF16).reshape(NP, 16, 128)
    hrecv[me] = hsend[me]
    local[1].wait()
    for s in range(3):
        rimsend[pl.ds(8 * s, 8), :] = fv[s, :, 384:].astype(F32).T[120:, :]

    pl.semaphore_wait(barrier, NP - 1 + 4)
    rim = pltpu.make_async_remote_copy(
        rimsend, rimrecv, osem.at[3], rsem.at[3],
        device_id={"ctx": lax.rem(me + 1, NP)}, device_id_type=MESH,
    )
    rim.start()

    def spread(send, recv, k, sem, far):
        def one(peer):
            pltpu.make_async_remote_copy(
                send.at[peer], recv.at[me], osem.at[k], sem,
                device_id={"ctx": peer}, device_id_type=MESH,
            ).start()

        visit(one, far)

    def arrived(part, sem):
        pltpu.make_async_copy(part, part, sem).wait()

    def mates(i, source, target):
        return pltpu.make_async_remote_copy(
            source, target, psem.at[i], prem.at[i], device_id={"ch": partner}, device_id_type=MESH
        )

    most = pl.ds(0, NP - 1)
    spread(hsend, hrecv, 0, rsem.at[0], False)
    local[4].wait()
    swap = mates(0, wv, wr)
    swap.start()

    local[2].wait()
    local[3].wait()
    cols[...] = jnp.zeros_like(cols)
    for s in range(3):
        for j in range(3):
            cols[pl.ds(3 * s + j, 1), :] = swv[s, pl.ds(j, 1), :]
    cols[pl.ds(9, 1), :] = skv[...]
    col = cols[...].T

    def short(s, edge, width):
        wide = jnp.concatenate([edge, fv[s, :, :width].astype(F32)], 1)
        total = col[:, 3 * s : 3 * s + 1] * wide[:, 128:]
        for j in (1, 2):
            moved = pltpu.roll(wide, j, 1)[:, 128:]
            total = total + col[:, 3 * s + j : 3 * s + j + 1] * moved
        return total

    nothing = jnp.zeros((128, 128), F32)
    gt[...] = short(1, nothing, 512) * short(2, nothing, 512)
    for a in range(1, 4):
        rows[pl.ds(a, 128, stride=4), :] = gt[:, 128 * a : 128 * a + 128]

    rim.wait()
    inside = me > 0

    def edge(s):
        last = jnp.concatenate([jnp.zeros((120, 128), F32), rimrecv[pl.ds(8 * s, 8), :]], 0)
        return jnp.where(inside, last.T, 0.0)

    gt[:, :128] = short(1, edge(1), 128) * short(2, edge(2), 128)
    rows[pl.ds(0, 128, stride=4), :] = gt[:, :128]
    gsend[...] = rows[...].astype(BF16).reshape(NP, 16, 128)
    grecv[me] = gsend[me]
    spread(gsend, grecv, 1, rsem.at[1], True)
    gt[...] = col[:, 9:10] * gt[...]
    f0[...] = short(0, edge(0), 512)

    for c in local[5:]:
        c.wait()
    arrived(hrecv.at[most], rsem.at[0])
    rows[...] = hrecv[...].reshape(512, 128).astype(F32)
    spec[...] = forward(rows, e1, m2, tw)
    swap.wait_recv()
    arrived(grecv.at[most], rsem.at[1])
    rows[...] = grecv[...].reshape(512, 128).astype(F32)
    inverse(product(forward(rows, e1, m2, tw), spec[...]), rows, m3, bk, tw)

    csend[...] = rows[...].astype(BF16).reshape(NP, 16, 128)
    crecv[me] = csend[me]
    spread(csend, crecv, 2, csem.at[z], False)

    planes = [lax.rem(z + d, 8) for d in (0, 1, 7, 2, 6, 3, 5, 4)]

    def hand(chip, k, t, other):
        piece = ag.at[chip, pl.ds(pl.multiple_of(16 * planes[k], 16), 16)]
        return pltpu.make_async_remote_copy(
            piece, piece, asem.at[t, k], arem.at[t, k], device_id={"ch": other}, device_id_type=MESH
        )

    sent = []

    def go(*args):
        copy = hand(*args)
        copy.start()
        sent.append(copy)

    def own(k):
        first = planes[k]
        arrived(crecv.at[pl.ds(0, 4 if k else 3)], csem.at[first])
        here = pl.ds(pl.multiple_of(16 * first, 16), 16)
        came = crecv[pl.ds(4 * first, 4)].reshape(64, 128)
        rows[pl.ds(64 * k, 64), :] = came.astype(F32)
        for a in range(4):
            lanes = pl.ds(128 * a, 128)
            conv = rows[pl.ds(64 * k + a, 16, stride=4), :]
            ag[y, here, lanes] = (f0[here, lanes] * (conv + gt[here, lanes])).astype(BF16)
        if k >= RELAYED:
            go(y, k, 2, across)
        go(y, k, k % 2, (up, down)[k % 2])
        go(y, k, 1 - k % 2, (down, up)[k % 2])

    taken = set()

    def take(t, k):
        if (t, k) not in taken:
            taken.add((t, k))
            other = (down, up, across)[t]
            hand(lax.div(other, 2), k, t, other).wait_recv()

    def relay(k):
        take(k % 2, k)
        go(lax.div((down, up)[k % 2], 2), k, 2, (up, down)[k % 2])

    for step in range(8 + LAG):
        if step < 8:
            own(step)
        if 0 <= step - LAG < RELAYED:
            relay(step - LAG)

    def term(chip):
        columns = pl.ds(pl.multiple_of(256 * chip + 128 * core, 128), 128)
        return dot(wr[:, columns], ag[chip]), dot(wv[:, columns], ag[chip])

    theirs, mine = term(y)
    for t, other in ((0, down), (1, up), (2, across)):
        for k in range(8):
            take(t, k)
        more = term(lax.div(other, 2))
        theirs, mine = theirs + more[0], mine + more[1]
    fin[...] = theirs
    last = mates(1, fin, finr)
    last.start()
    last.wait_recv()
    out[...] = (mine + finr[...]).astype(BF16)

    for copy in sent + [swap, last]:
        copy.wait_send()
    arrived(hsend.at[most], osem.at[0])
    arrived(gsend.at[most], osem.at[1])
    arrived(csend.at[most], osem.at[2])


def local(featurized, short_weights, filter_taps, skip_gain, w_out):
    e1, m2, m3, back, twist = tables()
    far = pl.BlockSpec(memory_space=pl.ANY)
    V = pltpu.VMEM
    chunk = V((NP, 16, 128), BF16)
    block = V((128, 512), F32)
    return pl.pallas_call(
        kernel,
        out_shape=jax.ShapeDtypeStruct((128, 512), BF16),
        in_specs=[far] * 10,
        out_specs=pl.BlockSpec(memory_space=pltpu.VMEM),
        scratch_shapes=[
            V((3, 128, 512), BF16), V((128, 512), F32), V((3, 3, 128), F32), V((1, 128), F32),
            V((128, 1024), BF16), V((128, 1024), BF16),
            V(e1.shape, BF16), V(m2.shape, BF16), V(m3.shape, BF16),
            V(back.shape, BF16), V(twist.shape, F32),
            V((24, 128), F32), V((24, 128), F32), V((128, 128), F32),
            block, block, V((512, 128), F32), chunk, chunk, chunk, chunk,
            chunk, chunk,
            V((512, 256), F32), V((4, 128, 512), BF16), block, block,
            pltpu.SemaphoreType.DMA((10,)),
            pltpu.SemaphoreType.DMA((4,)),
            pltpu.SemaphoreType.DMA((4,)),
            pltpu.SemaphoreType.DMA((8,)),
            pltpu.SemaphoreType.DMA((3, 8)),
            pltpu.SemaphoreType.DMA((3, 8)),
            pltpu.SemaphoreType.DMA((2,)),
            pltpu.SemaphoreType.DMA((2,)),
        ],
        compiler_params=pltpu.CompilerParams(collective_id=0, has_side_effects=True, vmem_limit_bytes=56350000),
        name="hyena",
    )(
        featurized, filter_taps, jnp.swapaxes(short_weights, 1, 2), skip_gain.reshape(1, 128),
        w_out, e1, m2, m3, back, twist,
    )


def solution(mesh):
    in_specs = (P(None, "ch", "ctx"), P(None, "ch", None), P("ch", "ctx"), P("ch"), P("ch", None))
    out_specs = P("ch", "ctx")
    return jax.shard_map(local, mesh=mesh, in_specs=in_specs, out_specs=out_specs, check_vma=False)
```

```python
import math

import jax
import jax.numpy as jnp
import numpy as np
from jax import lax
from jax.experimental import pallas as pl
from jax.experimental.pallas import tpu as pltpu
from jax.sharding import PartitionSpec as P

NP = 32
NC = 4
RELAYED, LAG = 6, 6
MESH = pl.DeviceIdType.MESH
F32 = jnp.float32
BF16 = jnp.bfloat16


def split(table):
    high = table.astype(BF16)
    return high, (table - high.astype(np.float32)).astype(BF16)


def tables():
    index = np.arange(128)
    first = 4 * (index % NP) + index // NP
    one = 2 * math.pi * (((4 * index[:, None] + 1) * first[None, :]) % 512) / 512
    two = 2 * math.pi * ((index[:, None] * index[None, :]) % 128) / 128
    twist = 2 * math.pi * (((4 * index[:, None] + 1) * index[None, :]) % 65536) / 65536
    c2, s2 = np.cos(two), np.sin(two)
    f32 = np.float32
    e1 = np.concatenate([np.cos(one), -np.sin(one)], 0).astype(f32)
    m2 = np.block([[c2, -s2], [s2, c2]]).astype(f32)
    m3 = np.block([[c2, s2], [-s2, c2]]).astype(f32)
    back = (np.concatenate([np.cos(one).T, -np.sin(one).T], 1) / 16384).astype(f32)
    e1_high, e1_low = split(e1)
    return (
        np.concatenate([e1_high, e1_low], 1),
        np.stack(split(m2)),
        np.stack(split(m3)),
        np.stack(split(back)),
        np.stack([np.cos(twist), -np.sin(twist)]).astype(f32),
    )


def dot(left, right):
    return jnp.dot(left, right, preferred_element_type=F32)


def halves(value):
    high = value.astype(BF16)
    return high, (value - high.astype(F32)).astype(BF16)


def forward(rows, e1, m2, twist):
    parts = []
    for c in range(NC):
        parts.append(
            jnp.concatenate([rows[pl.ds(4 * c + a, NP, stride=16), :] for a in range(4)], 0)
        )
    grid = jnp.concatenate(parts, 1).astype(BF16)
    mixed = dot(e1[...], jnp.concatenate([grid, grid], 0))
    tr, ti = twist[0], twist[1]
    turned = []
    for c in range(NC):
        re, im = mixed[:128, 128 * c : 128 * c + 128], mixed[128:, 128 * c : 128 * c + 128]
        turned.append(jnp.concatenate([re * tr - im * ti, re * ti + im * tr], 1))
    high, low = halves(jnp.concatenate(turned, 0))
    return dot(jnp.concatenate([high, low, high], 1), jnp.concatenate([m2[0], m2[0], m2[1]], 0))


def inverse(spectrum, rows, m3, back, twist):
    high, low = halves(spectrum)
    mixed = dot(jnp.concatenate([high, low, high], 1), jnp.concatenate([m3[0], m3[0], m3[1]], 0))
    tr, ti = twist[0], twist[1]
    turned = []
    for c in range(NC):
        re, im = mixed[128 * c : 128 * c + 128, :128], mixed[128 * c : 128 * c + 128, 128:]
        turned.append(jnp.concatenate([re * tr + im * ti, im * tr - re * ti], 0))
    high, low = halves(jnp.concatenate(turned, 1))
    done = dot(jnp.concatenate([back[0], back[1], back[0]], 1), jnp.concatenate([high, high, low], 0))
    for c in range(NC):
        for a in range(4):
            rows[pl.ds(4 * c + a, NP, stride=16), :] = done[
                NP * a : NP * a + NP, 128 * c : 128 * c + 128
            ]


def product(g, h):
    gr, gi, hr, hi = g[:, :128], g[:, 128:], h[:, :128], h[:, 128:]
    return jnp.concatenate([gr * hr - gi * hi, gr * hi + gi * hr], 1)


def plane_order(k):
    return lax.div(k + 1, 2) * (2 * lax.rem(k, 2) - 1)


def kernel(
    feat, taps, sw, skip, w, e1h, m2h, m3h, bkh, twh, out,
    fv, tv, swv, skv, wv, wr, e1, m2, m3, bk, tw,
    rimsend, rimrecv, cols, f0, gt, rows,
    hsend, hrecv, gsend, grecv, csend, crecv, spec, ag, fin, finr,
    lsem, osem, rsem, csem, asem, arem, psem, prem,
):
    me = lax.axis_index("ctx")
    ch = lax.axis_index("ch")
    x, z = lax.rem(me, 4), lax.div(me, 4)
    y, core = lax.div(ch, 2), lax.rem(ch, 2)
    partner = 2 * y + 1 - core
    up, down, across = (2 * lax.rem(y + d, 4) + core for d in (1, 3, 2))
    row = [lax.rem(x + d, 4) for d in range(4)]

    def plane(k):
        return lax.rem(z + 8 + plane_order(k), 8)

    def visit(do, far):
        def one(k, _):
            base = 4 * plane(8 - k if far else k)
            for d in (2, 1, 3, 0):
                do(base + row[d])
            return 0

        def own():
            for d in (2, 1, 3):
                do(4 * z + row[d])

        if not far:
            own()
        lax.fori_loop(1, 8, one, 0)
        if far:
            own()

    local = [
        pltpu.make_async_copy(s, d, lsem.at[i])
        for i, (s, d) in enumerate(
            [(taps, tv), (feat, fv), (sw, swv), (skip, skv), (w, wv), (e1h, e1), (m2h, m2), (twh, tw),
             (m3h, m3), (bkh, bk)]
        )
    ]
    barrier = pltpu.get_barrier_semaphore()

    def greet(peer):
        pl.semaphore_signal(barrier, inc=1, device_id={"ctx": peer}, device_id_type=MESH)

    visit(greet, True)
    for other in (partner, up, down, across):
        pl.semaphore_signal(barrier, inc=1, device_id={"ch": other}, device_id_type=MESH)
    for c in local:
        c.start()

    local[0].wait()
    for a in range(4):
        rows[pl.ds(a, 128, stride=4), :] = tv[:, 128 * a : 128 * a + 128]
    hsend[...] = rows[...].astype(BF16).reshape(NP, 16, 128)
    hrecv[me] = hsend[me]
    local[1].wait()
    for s in range(3):
        rimsend[pl.ds(8 * s, 8), :] = fv[s, :, 384:].astype(F32).T[120:, :]

    local[2].wait()
    local[3].wait()
    cols[...] = jnp.zeros_like(cols)
    for s in range(3):
        for j in range(3):
            cols[pl.ds(3 * s + j, 1), :] = swv[s, pl.ds(j, 1), :]
    cols[pl.ds(9, 1), :] = skv[...]
    col = cols[...].T

    def short(s, edge, width):
        wide = jnp.concatenate([edge, fv[s, :, :width].astype(F32)], 1)
        total = col[:, 3 * s : 3 * s + 1] * wide[:, 128:]
        for j in (1, 2):
            moved = pltpu.roll(wide, j, 1)[:, 128:]
            total = total + col[:, 3 * s + j : 3 * s + j + 1] * moved
        return total

    nothing = jnp.zeros((128, 128), F32)
    gt[...] = short(1, nothing, 512) * short(2, nothing, 512)
    for a in range(1, 4):
        rows[pl.ds(a, 128, stride=4), :] = gt[:, 128 * a : 128 * a + 128]

    pl.semaphore_wait(barrier, NP - 1 + 4)
    rim = pltpu.make_async_remote_copy(
        rimsend, rimrecv, osem.at[3], rsem.at[3],
        device_id={"ctx": lax.rem(me + 1, NP)}, device_id_type=MESH,
    )
    rim.start()

    def spread(send, recv, k, sem, far):
        def one(peer):
            pltpu.make_async_remote_copy(
                send.at[peer], recv.at[me], osem.at[k], sem,
                device_id={"ctx": peer}, device_id_type=MESH,
            ).start()

        visit(one, far)

    def arrived(part, sem):
        pltpu.make_async_copy(part, part, sem).wait()

    def mates(i, source, target):
        return pltpu.make_async_remote_copy(
            source, target, psem.at[i], prem.at[i], device_id={"ch": partner}, device_id_type=MESH
        )

    most = pl.ds(0, NP - 1)
    spread(hsend, hrecv, 0, rsem.at[0], False)
    local[4].wait()
    swap = mates(0, wv, wr)
    swap.start()

    rim.wait()
    inside = me > 0

    def edge(s):
        last = jnp.concatenate([jnp.zeros((120, 128), F32), rimrecv[pl.ds(8 * s, 8), :]], 0)
        return jnp.where(inside, last.T, 0.0)

    gt[:, :128] = short(1, edge(1), 128) * short(2, edge(2), 128)
    rows[pl.ds(0, 128, stride=4), :] = gt[:, :128]
    gsend[...] = rows[...].astype(BF16).reshape(NP, 16, 128)
    grecv[me] = gsend[me]
    spread(gsend, grecv, 1, rsem.at[1], True)
    gt[...] = col[:, 9:10] * gt[...]
    f0[...] = short(0, edge(0), 512)

    for c in local[5:]:
        c.wait()
    arrived(hrecv.at[most], rsem.at[0])
    rows[...] = hrecv[...].reshape(512, 128).astype(F32)
    spec[...] = forward(rows, e1, m2, tw)
    swap.wait_recv()
    arrived(grecv.at[most], rsem.at[1])
    rows[...] = grecv[...].reshape(512, 128).astype(F32)
    inverse(product(forward(rows, e1, m2, tw), spec[...]), rows, m3, bk, tw)

    csend[...] = rows[...].astype(BF16).reshape(NP, 16, 128)
    crecv[me] = csend[me]
    spread(csend, crecv, 2, csem.at[z], False)

    planes = [lax.rem(z + d, 8) for d in (0, 1, 7, 2, 6, 3, 5, 4)]

    def hand(chip, k, t, other):
        piece = ag.at[chip, pl.ds(pl.multiple_of(16 * planes[k], 16), 16)]
        return pltpu.make_async_remote_copy(
            piece, piece, asem.at[t, k], arem.at[t, k], device_id={"ch": other}, device_id_type=MESH
        )

    sent = []

    def go(*args):
        copy = hand(*args)
        copy.start()
        sent.append(copy)

    def own(k):
        first = planes[k]
        arrived(crecv.at[pl.ds(0, 4 if k else 3)], csem.at[first])
        here = pl.ds(pl.multiple_of(16 * first, 16), 16)
        came = crecv[pl.ds(4 * first, 4)].reshape(64, 128)
        rows[pl.ds(64 * k, 64), :] = came.astype(F32)
        for a in range(4):
            lanes = pl.ds(128 * a, 128)
            conv = rows[pl.ds(64 * k + a, 16, stride=4), :]
            ag[y, here, lanes] = (f0[here, lanes] * (conv + gt[here, lanes])).astype(BF16)
        if k >= RELAYED:
            go(y, k, 2, across)
        go(y, k, k % 2, (up, down)[k % 2])
        go(y, k, 1 - k % 2, (down, up)[k % 2])

    taken = set()

    def take(t, k):
        if (t, k) not in taken:
            taken.add((t, k))
            other = (down, up, across)[t]
            hand(lax.div(other, 2), k, t, other).wait_recv()

    def relay(k):
        take(k % 2, k)
        go(lax.div((down, up)[k % 2], 2), k, 2, (up, down)[k % 2])

    for step in range(8 + LAG):
        if step < 8:
            own(step)
        if 0 <= step - LAG < RELAYED:
            relay(step - LAG)

    def term(chip):
        columns = pl.ds(pl.multiple_of(256 * chip + 128 * core, 128), 128)
        return dot(wr[:, columns], ag[chip]), dot(wv[:, columns], ag[chip])

    theirs, mine = term(y)
    for t, other in ((0, down), (1, up), (2, across)):
        for k in range(8):
            take(t, k)
        more = term(lax.div(other, 2))
        theirs, mine = theirs + more[0], mine + more[1]
    fin[...] = theirs
    last = mates(1, fin, finr)
    last.start()
    last.wait_recv()
    out[...] = (mine + finr[...]).astype(BF16)

    for copy in sent + [swap, last]:
        copy.wait_send()
    arrived(hsend.at[most], osem.at[0])
    arrived(gsend.at[most], osem.at[1])
    arrived(csend.at[most], osem.at[2])


def local(featurized, short_weights, filter_taps, skip_gain, w_out):
    e1, m2, m3, back, twist = tables()
    far = pl.BlockSpec(memory_space=pl.ANY)
    V = pltpu.VMEM
    chunk = V((NP, 16, 128), BF16)
    block = V((128, 512), F32)
    return pl.pallas_call(
        kernel,
        out_shape=jax.ShapeDtypeStruct((128, 512), BF16),
        in_specs=[far] * 10,
        out_specs=pl.BlockSpec(memory_space=pltpu.VMEM),
        scratch_shapes=[
            V((3, 128, 512), BF16), V((128, 512), F32), V((3, 3, 128), F32), V((1, 128), F32),
            V((128, 1024), BF16), V((128, 1024), BF16),
            V(e1.shape, BF16), V(m2.shape, BF16), V(m3.shape, BF16),
            V(back.shape, BF16), V(twist.shape, F32),
            V((24, 128), F32), V((24, 128), F32), V((128, 128), F32),
            block, block, V((512, 128), F32), chunk, chunk, chunk, chunk,
            chunk, chunk,
            V((512, 256), F32), V((4, 128, 512), BF16), block, block,
            pltpu.SemaphoreType.DMA((10,)),
            pltpu.SemaphoreType.DMA((4,)),
            pltpu.SemaphoreType.DMA((4,)),
            pltpu.SemaphoreType.DMA((8,)),
            pltpu.SemaphoreType.DMA((3, 8)),
            pltpu.SemaphoreType.DMA((3, 8)),
            pltpu.SemaphoreType.DMA((2,)),
            pltpu.SemaphoreType.DMA((2,)),
        ],
        compiler_params=pltpu.CompilerParams(collective_id=0, has_side_effects=True, vmem_limit_bytes=56350000),
        name="hyena",
    )(
        featurized, filter_taps, jnp.swapaxes(short_weights, 1, 2), skip_gain.reshape(1, 128),
        w_out, e1, m2, m3, back, twist,
    )


def solution(mesh):
    in_specs = (P(None, "ch", "ctx"), P(None, "ch", None), P("ch", "ctx"), P("ch"), P("ch", None))
    out_specs = P("ch", "ctx")
    return jax.shard_map(local, mesh=mesh, in_specs=in_specs, out_specs=out_specs, check_vma=False)
```
